256 devices in a mesh: stage: 32 (over z, y), expert: 8 (over x, core).
Axes of the slice: x: 4, y: 4, z: 8, core: 2. Of those that a mesh axis runs over, the one named last changes fastest.
Arguments:
- x_act: bfloat16 [32, 6144, 512], P('stage', 'expert')
- route_idx: int32 [32, 6144, 2], P('stage', 'expert')
- route_gate: float32 [32, 6144, 2], P('stage', 'expert')
- w_up: bfloat16 [32, 8, 512, 256], P('stage', 'expert')
- w_lin: bfloat16 [32, 8, 512, 256], P('stage', 'expert')
- w_down: bfloat16 [32, 8, 256, 512], P('stage', 'expert')
- dy_out: bfloat16 [32, 6144, 512], P('stage', 'expert')
Outputs:
- output 1: bfloat16 [32, 6144, 512], P('stage', 'expert')
- output 2: bfloat16 [32, 6144, 512], P('stage', 'expert')
- output 3: bfloat16 [32, 8, 512, 256], P('stage', 'expert')
- output 4: bfloat16 [32, 8, 512, 256], P('stage', 'expert')
- output 5: bfloat16 [32, 8, 256, 512], P('stage', 'expert')
All inputs are finite; a program needn't handle non-finite values.
Results may differ from the reference program's by a relative error of at most 0.001.
Values are sent between devices in bfloat16 or wider.
A program may use at most 768 MiB of HBM per device.

```python
import jax
import jax.numpy as jnp
from jax import lax

STAGE_DEVS = 32
EXPERT_DEVS = 8
TOKENS = 768
D_MODEL = 512
D_FF = 256
EXPERTS = 8
TOP_K = 2

CAPACITY = 4 * TOKENS // EXPERTS
ROWS = EXPERT_DEVS * TOKENS


def draw_routing(rng_key):
    key_hot, key_bias, key_cell, key_perm, key_swap = jax.random.split(rng_key, 5)
    num_cells = EXPERTS * CAPACITY
    cell_ids = jnp.arange(num_cells, dtype=jnp.int32)
    cell_expert = cell_ids // CAPACITY
    cell_slot = cell_ids % CAPACITY
    hot_expert = jax.random.randint(key_hot, (), 0, EXPERTS)
    expert_bias = jax.random.randint(key_bias, (EXPERTS,), 0, 4) * 256
    cell_score = jax.random.randint(key_cell, (num_cells,), 0, 1024) + expert_bias[cell_expert]
    needed = (cell_slot == 0) | (cell_expert == hot_expert)
    cell_score = jnp.where(needed, 4096, cell_score)
    top_vals, chosen = lax.top_k(cell_score * num_cells + cell_ids, 2 * TOKENS)
    chosen_expert = jnp.sort(chosen) // CAPACITY
    expert_pairs = jnp.stack([chosen_expert[:TOKENS], chosen_expert[TOKENS:]], axis=1)
    expert_pairs = expert_pairs[jax.random.permutation(key_perm, TOKENS)]
    swap_flag = jax.random.randint(key_swap, (TOKENS, 1), 0, 2)
    return jnp.where(swap_flag == 1, expert_pairs[:, ::-1], expert_pairs).astype(jnp.int32)


def setup_inputs(seed: int = 0) -> dict:
    root_key = jax.random.key(seed)
    key_x, key_route, key_gate, key_up, key_lin, key_down, key_dy = jax.random.split(root_key, 7)
    shape_tok = (STAGE_DEVS, ROWS, D_MODEL)
    x_act = jax.random.normal(key_x, shape_tok, jnp.float32).astype(jnp.bfloat16)
    route_keys = jax.random.split(key_route, STAGE_DEVS * EXPERT_DEVS)
    route_idx = jax.vmap(draw_routing)(route_keys).reshape(STAGE_DEVS, ROWS, TOP_K)
    first_gate = jax.random.uniform(key_gate, (STAGE_DEVS, ROWS, 1), jnp.float32, 0.3, 0.7)
    route_gate = jnp.concatenate([first_gate, 1.0 - first_gate], axis=-1)
    shape_in = (STAGE_DEVS, EXPERTS, D_MODEL, D_FF)
    shape_out = (STAGE_DEVS, EXPERTS, D_FF, D_MODEL)
    w_up = (jax.random.normal(key_up, shape_in, jnp.float32) * D_MODEL ** -0.5).astype(jnp.bfloat16)
    w_lin = (jax.random.normal(key_lin, shape_in, jnp.float32) * D_MODEL ** -0.5).astype(jnp.bfloat16)
    w_down = (jax.random.normal(key_down, shape_out, jnp.float32) * D_FF ** -0.5).astype(jnp.bfloat16)
    dy_out = jax.random.normal(key_dy, shape_tok, jnp.float32).astype(jnp.bfloat16)
    return {"x_act": x_act, "route_idx": route_idx, "route_gate": route_gate, "w_up": w_up, "w_lin": w_lin, "w_down": w_down, "dy_out": dy_out}


def expert_block(x_src, idx_src, gate_src, dy_dst, w_up, w_lin, w_down):
    member = jnp.sum(jax.nn.one_hot(idx_src, EXPERTS, dtype=jnp.int32), axis=1)
    earlier = jnp.cumsum(member, axis=0) - member
    slot_pos = jnp.take_along_axis(earlier, idx_src, axis=1)
    x_copies = jnp.broadcast_to(x_src.astype(jnp.float32)[:, None, :], (TOKENS, TOP_K, D_MODEL))
    empty_rows = jnp.zeros((EXPERTS, CAPACITY, D_MODEL), jnp.float32)
    x_rows = empty_rows.at[idx_src, slot_pos].set(x_copies)
    pre_up = jnp.einsum("ecd,edf->ecf", x_rows, w_up)
    pre_lin = jnp.einsum("ecd,edf->ecf", x_rows, w_lin)
    act_up = jax.nn.silu(pre_up)
    hidden = (act_up * pre_lin).astype(jnp.bfloat16).astype(jnp.float32)
    out_rows = jnp.einsum("ecf,efd->ecd", hidden, w_down).astype(jnp.bfloat16).astype(jnp.float32)
    out_copies = out_rows[idx_src, slot_pos]
    y_tok = jnp.sum(gate_src[:, :, None] * out_copies, axis=1).astype(jnp.bfloat16)
    d_copies = (gate_src[:, :, None] * dy_dst.astype(jnp.float32)[:, None, :]).astype(jnp.bfloat16).astype(jnp.float32)
    d_rows = empty_rows.at[idx_src, slot_pos].set(d_copies)
    d_hidden = jnp.einsum("ecd,efd->ecf", d_rows, w_down).astype(jnp.bfloat16).astype(jnp.float32)
    sigmoid_up = jax.nn.sigmoid(pre_up)
    d_up = (d_hidden * pre_lin * sigmoid_up * (1.0 + pre_up * (1.0 - sigmoid_up))).astype(jnp.bfloat16).astype(jnp.float32)
    d_lin = (d_hidden * act_up).astype(jnp.bfloat16).astype(jnp.float32)
    g_up = jnp.einsum("ecd,ecf->edf", x_rows, d_up)
    g_lin = jnp.einsum("ecd,ecf->edf", x_rows, d_lin)
    g_down = jnp.einsum("ecf,ecd->efd", hidden, d_rows)
    dx_rows = (jnp.einsum("ecf,edf->ecd", d_up, w_up) + jnp.einsum("ecf,edf->ecd", d_lin, w_lin)).astype(jnp.bfloat16).astype(jnp.float32)
    dx_tok = jnp.sum(dx_rows[idx_src, slot_pos], axis=1).astype(jnp.bfloat16)
    return y_tok, dx_tok, g_up, g_lin, g_down


def stage_block(stage_args):
    x_stage, idx_stage, gate_stage, dy_stage, w_up, w_lin, w_down = stage_args
    w_up32 = w_up.astype(jnp.float32)
    w_lin32 = w_lin.astype(jnp.float32)
    w_down32 = w_down.astype(jnp.float32)

    def device_step(grad_sums, dev_block):
        block_out = expert_block(dev_block[0], dev_block[1], dev_block[2], dev_block[3], w_up32, w_lin32, w_down32)
        new_sums = (grad_sums[0] + block_out[2], grad_sums[1] + block_out[3], grad_sums[2] + block_out[4])
        return new_sums, (block_out[0], block_out[1])

    zero_grads = (jnp.zeros((EXPERTS, D_MODEL, D_FF), jnp.float32), jnp.zeros((EXPERTS, D_MODEL, D_FF), jnp.float32), jnp.zeros((EXPERTS, D_FF, D_MODEL), jnp.float32))
    dev_blocks = (x_stage.reshape(EXPERT_DEVS, TOKENS, D_MODEL), idx_stage.reshape(EXPERT_DEVS, TOKENS, TOP_K), gate_stage.reshape(EXPERT_DEVS, TOKENS, TOP_K), dy_stage.reshape(EXPERT_DEVS, TOKENS, D_MODEL))
    grad_sums, tok_outs = lax.scan(device_step, zero_grads, dev_blocks)
    y_stage = tok_outs[0].reshape(ROWS, D_MODEL)
    dx_stage = tok_outs[1].reshape(ROWS, D_MODEL)
    return y_stage, dx_stage, grad_sums[0].astype(jnp.bfloat16), grad_sums[1].astype(jnp.bfloat16), grad_sums[2].astype(jnp.bfloat16)


def reference(x_act, route_idx, route_gate, w_up, w_lin, w_down, dy_out):
    x_from = jnp.roll(x_act, 1, axis=0)
    idx_from = jnp.roll(route_idx, 1, axis=0)
    gate_from = jnp.roll(route_gate, 1, axis=0)
    y_out, dx_next, dw_up, dw_lin, dw_down = lax.map(stage_block, (x_from, idx_from, gate_from, dy_out, w_up, w_lin, w_down))
    dx_act = jnp.roll(dx_next, -1, axis=0)
    return y_out, dx_act, dw_up, dw_lin, dw_down
```

```python
import jax
import jax.numpy as jnp
from jax import lax
from jax.sharding import PartitionSpec as P

F32 = jnp.float32
BF16 = jnp.bfloat16


def dense_gates(idx_tok, gate_tok, num_experts):
    hit = idx_tok[:, :, None] == jnp.arange(num_experts, dtype=jnp.int32)
    return jnp.sum(jnp.where(hit, gate_tok[:, :, None], 0.0), axis=1)


def expert_acts(x_rows, u_rows, routed, w_up, w_lin, w_down):
    pre_up = jnp.where(routed, jnp.dot(x_rows, w_up, preferred_element_type=F32), 0.0)
    pre_lin = jnp.where(routed, jnp.dot(x_rows, w_lin, preferred_element_type=F32), 0.0)
    sig = jax.nn.sigmoid(pre_up)
    act = pre_up * sig
    hidden = (act * pre_lin).astype(BF16)
    d_hid = lax.dot_general(u_rows, w_down, (((1,), (1,)), ((), ())), preferred_element_type=F32).astype(BF16).astype(F32)
    d_up = (d_hid * pre_lin * sig * (1.0 + pre_up * (1.0 - sig))).astype(BF16)
    d_lin = (d_hid * act).astype(BF16)
    return hidden, d_up, d_lin


def tdot(a, b):
    return lax.dot_general(a, b, (((0,), (0,)), ((), ())), preferred_element_type=F32)


def ndot(a, b):
    return lax.dot_general(a, b, (((1,), (1,)), ((), ())), preferred_element_type=F32)


def solution(mesh):
    stages = mesh.shape["stage"]
    groups = mesh.shape["expert"]
    send_next = [(src, (src + 1) % stages) for src in range(stages)]
    send_back = [(src, (src - 1) % stages) for src in range(stages)]
    tok_spec = P("stage", "expert", None)
    w_spec = P("stage", "expert", None, None)

    def device_step(x_act, route_idx, route_gate, w_up, w_lin, w_down, dy_out):
        num_experts = w_up.shape[1] * groups
        me = lax.axis_index("expert")
        gates = dense_gates(route_idx[0], route_gate[0], num_experts)
        x_tok = lax.ppermute(x_act[0], "stage", send_next)
        g_tok = lax.ppermute(gates.T, "stage", send_next)
        w_pack = jnp.concatenate([w_up[0, 0], w_lin[0, 0], w_down[0, 0].reshape(512, 256)], axis=0)
        w_all = lax.all_gather(w_pack, "expert")
        dy_all = lax.all_gather(dy_out[0], "expert", tiled=True)
        x_all = lax.all_gather(x_tok, "expert", tiled=True)
        g_all = lax.all_gather(g_tok, "expert")
        g_mine = lax.dynamic_index_in_dim(g_all, me, 1, keepdims=False).reshape(-1)[:, None]
        g_own = g_tok.T
        dy = dy_out[0]
        y_acc = 0.0
        dx_acc = 0.0
        for e in range(num_experts):
            gate = g_own[:, e:e + 1]
            w_u, w_l, w_d = w_all[e, :512], w_all[e, 512:1024], w_all[e, 1024:].reshape(256, 512)
            u_rows = (gate * dy.astype(F32)).astype(BF16)
            hidden, d_up, d_lin = expert_acts(x_tok, u_rows, gate > 0.0, w_u, w_l, w_d)
            out = jnp.dot(hidden, w_d, preferred_element_type=F32).astype(BF16).astype(F32)
            y_acc = y_acc + gate * out
            dx_acc = dx_acc + (ndot(d_up, w_u) + ndot(d_lin, w_l)).astype(BF16).astype(F32)
        dx_prev = lax.ppermute(dx_acc.astype(BF16), "stage", send_back)
        u_all = (g_mine * dy_all.astype(F32)).astype(BF16)
        hidden, d_up, d_lin = expert_acts(x_all, u_all, g_mine > 0.0, w_up[0, 0], w_lin[0, 0], w_down[0, 0])
        g_up = tdot(x_all, d_up).astype(BF16)
        g_lin = tdot(x_all, d_lin).astype(BF16)
        g_down = tdot(hidden, u_all).astype(BF16)
        return y_acc.astype(BF16)[None], dx_prev[None], g_up[None, None], g_lin[None, None], g_down[None, None]

    return jax.shard_map(device_step, mesh=mesh, in_specs=(tok_spec, tok_spec, tok_spec, w_spec, w_spec, w_spec, tok_spec), out_specs=(tok_spec, tok_spec, w_spec, w_spec, w_spec), check_vma=False)
```

```python
import functools

import jax
import jax.numpy as jnp
from jax import lax
from jax.experimental import pallas as pl
from jax.experimental.pallas import tpu as pltpu
from jax.sharding import PartitionSpec as P

F32 = jnp.float32
BF16 = jnp.bfloat16
MESH = pl.DeviceIdType.MESH

OWN, SIB, LEFT, LEFT_SIB, RIGHT, RIGHT_SIB, OPP, OPP_SIB = range(8)


def cols(gate, width):
    return jnp.concatenate([gate] * (width // 128), axis=1)


def nt_dot(a, b):
    return lax.dot_general(a, b, (((1,), (1,)), ((), ())), preferred_element_type=F32)


def tn_dot(a, b):
    return lax.dot_general(a, b, (((0,), (0,)), ((), ())), preferred_element_type=F32)


def nn_dot(a, b):
    return jnp.dot(a, b, preferred_element_type=F32)


def expert_math(x_rows, dy_rows, gate, w_ul, w_down):
    ff = w_down.shape[0]
    routed = cols(gate, ff) > 0.0
    pre = nn_dot(x_rows, w_ul)
    pre_up = jnp.where(routed, pre[:, :ff], 0.0)
    pre_lin = jnp.where(routed, pre[:, ff:], 0.0)
    sig = 1.0 / (1.0 + jnp.exp(-pre_up))
    act = pre_up * sig
    hidden = (act * pre_lin).astype(BF16)
    u_rows = (cols(gate, dy_rows.shape[1]) * dy_rows.astype(F32)).astype(BF16)
    d_hid = nt_dot(u_rows, w_down).astype(BF16).astype(F32)
    d_up = (d_hid * pre_lin * sig * (1.0 + pre_up * (1.0 - sig))).astype(BF16)
    d_lin = (d_hid * act).astype(BF16)
    return hidden, u_rows, jnp.concatenate([d_up, d_lin], axis=1)


def moe_kernel(
    stages, groups, x_hbm, idx_hbm, gate_hbm, up_hbm, lin_hbm, down_hbm, dy_hbm,
    y_hbm, dx_hbm, dup_ref, dlin_ref, ddown_ref,
    w_all, d_all, x_all, idx_all, gate_all, gate_own, gate_exp, y_acc, dx_acc, y_buf, dx_buf, dul_acc, ddown_acc,
    load_sem, send_sem, recv_sem, small_send, small_recv, shift_send, shift_recv, out_sem,
):
    tokens, d_model = x_hbm.shape
    ff = down_hbm.shape[0]
    half, quarter = tokens // 2, tokens // 4
    stage, expert = lax.axis_index("stage"), lax.axis_index("expert")
    core = lax.rem(expert, 2)
    right = {"expert": lax.rem(expert + 2, groups)}
    left = {"expert": lax.rem(expert + groups - 2, groups)}
    sib = {"expert": expert + 1 - 2 * core}
    after = {"stage": lax.rem(stage + 1, stages)}
    before = {"stage": lax.rem(stage + stages - 1, stages)}

    loads = [
        pltpu.make_async_copy(up_hbm, w_all.at[OWN, pl.ds(0, d_model), pl.ds(0, ff)], load_sem.at[0]),
        pltpu.make_async_copy(lin_hbm, w_all.at[OWN, pl.ds(0, d_model), pl.ds(ff, ff)], load_sem.at[1]),
        pltpu.make_async_copy(down_hbm, w_all.at[OWN, pl.ds(d_model, ff)], load_sem.at[2]),
        pltpu.make_async_copy(dy_hbm, d_all.at[OWN], load_sem.at[3]),
    ]
    for load in loads:
        load.start()

    barrier = pltpu.get_barrier_semaphore()
    for peer in (right, left, sib, after, before):
        pl.semaphore_signal(barrier, inc=1, device_id=peer, device_id_type=MESH)
    pl.semaphore_wait(barrier, 5)

    started = []

    def remote(src, dst, send, recv, peer):
        return pltpu.make_async_remote_copy(src_ref=src, dst_ref=dst, send_sem=send, recv_sem=recv, device_id=peer, device_id_type=MESH)

    arrays = (w_all, d_all, x_all)
    kinds = [
        (OWN, LEFT, 0, half, right), (OWN, LEFT, half, half, right),
        (OWN, RIGHT, half, half, left), (OWN, RIGHT, 0, half, left),
        (OWN, SIB, 0, tokens, sib),
        (LEFT, OPP, 0, quarter, right), (LEFT, OPP, quarter, quarter, right),
        (RIGHT, OPP, half, quarter, left), (RIGHT, OPP, half + quarter, quarter, left),
        (LEFT, LEFT_SIB, 0, half, sib), (LEFT, LEFT_SIB, half, half, sib),
        (RIGHT, RIGHT_SIB, half, half, sib), (RIGHT, RIGHT_SIB, 0, half, sib),
        (OPP, OPP_SIB, 0, quarter, sib), (OPP, OPP_SIB, quarter, quarter, sib),
        (OPP, OPP_SIB, half, quarter, sib), (OPP, OPP_SIB, half + quarter, quarter, sib),
    ]

    def block_copy(array, kind):
        src_slot, dst_slot, row, rows, peer = kinds[kind]
        ref = arrays[array]
        return remote(
            ref.at[src_slot, pl.ds(row, rows)], ref.at[dst_slot, pl.ds(row, rows)],
            send_sem.at[array, kind], recv_sem.at[array, kind], peer,
        )

    def send(array, *which):
        for kind in which:
            copy = block_copy(array, kind)
            copy.start()
            started.append(copy)

    def arrive(array, *which):
        for kind in which:
            block_copy(array, kind).wait_recv()

    small = [(OWN, LEFT, right), (OWN, RIGHT, left), (OWN, SIB, sib), (LEFT, OPP, right), (LEFT, LEFT_SIB, sib), (RIGHT, RIGHT_SIB, sib), (OPP, OPP_SIB, sib)]

    def small_copies(kind):
        src_slot, dst_slot, peer = small[kind]
        return [
            remote(ref.at[src_slot], ref.at[dst_slot], small_send.at[which, kind], small_recv.at[which, kind], peer)
            for which, ref in enumerate((idx_all, gate_all))
        ]

    def send_small(*which):
        for kind in which:
            for copy in small_copies(kind):
                copy.start()
                started.append(copy)

    def arrive_small(*which):
        for kind in which:
            for copy in small_copies(kind):
                copy.wait_recv()

    shifts = [
        remote(idx_hbm, idx_all.at[OWN], shift_send.at[0], shift_recv.at[0], after),
        remote(gate_hbm, gate_all.at[OWN], shift_send.at[1], shift_recv.at[1], after),
        remote(x_hbm, x_all.at[OWN], shift_send.at[2], shift_recv.at[2], after),
    ]
    for copy in shifts:
        copy.start()
        started.append(copy)
    for load in loads:
        load.wait()
    send(0, 0, 2, 1, 3, 4)
    send(1, 0, 2, 1, 3, 4)

    def gate_columns(slot, expert_id):
        ids, gates = idx_all[slot], gate_all[slot]
        row = jnp.sum(jnp.where(ids == expert_id, gates, 0.0), axis=0, keepdims=True)
        return jnp.broadcast_to(row, (128, tokens)).T

    def expert_at(slot):
        chip_step = (0, 0, groups - 2, groups - 2, 2, 2, 4, 4)[slot]
        flip = (1 - 2 * core) if slot % 2 else 0
        return lax.rem(expert + flip + chip_step, groups)

    shifts[0].wait_recv()
    shifts[1].wait_recv()
    send_small(2, 0, 1)
    for slot in range(8):
        gate_own[slot] = gate_columns(OWN, expert_at(slot))
    gate_exp[OWN] = gate_columns(OWN, expert)
    y_acc[...] = jnp.zeros_like(y_acc)
    dx_acc[...] = jnp.zeros_like(dx_acc)
    dul_acc[...] = jnp.zeros_like(dul_acc)
    ddown_acc[...] = jnp.zeros_like(ddown_acc)
    arrive_small(2)
    gate_exp[SIB] = gate_columns(SIB, expert)

    def owner(first, last):
        def body(step, carry):
            slot = first + step // 2
            rows = pl.ds(pl.multiple_of(lax.rem(step, 2) * half, half), half)
            w_ul, w_down = w_all[slot, pl.ds(0, d_model)], w_all[slot, pl.ds(d_model, ff)]
            gate = gate_own[slot, rows]
            hidden, _, d_ul = expert_math(x_all[OWN, rows], d_all[OWN, rows], gate, w_ul, w_down)
            out = nn_dot(hidden, w_down).astype(BF16).astype(F32)
            y_acc[rows] += cols(gate, d_model) * out
            dx_acc[rows] += nt_dot(d_ul, w_ul).astype(BF16).astype(F32)
            return carry

        lax.fori_loop(0, 2 * (last - first), body, 0)

    def expert_rows(slot, rows):
        w_ul, w_down = w_all[OWN, pl.ds(0, d_model)], w_all[OWN, pl.ds(d_model, ff)]
        x_rows = x_all[slot, rows]
        hidden, u_rows, d_ul = expert_math(x_rows, d_all[slot, rows], gate_exp[slot, rows], w_ul, w_down)
        dul_acc[...] += tn_dot(x_rows, d_ul)
        ddown_acc[...] += tn_dot(hidden, u_rows)

    def expert_blocks(first, last):
        def body(step, carry):
            expert_rows(first + step // 2, pl.ds(pl.multiple_of(lax.rem(step, 2) * half, half), half))
            return carry

        lax.fori_loop(0, 2 * (last - first), body, 0)

    arrive(0, 0, 2)
    send(0, 5, 6, 7, 8, 9, 11)
    arrive(0, 1, 3)
    send(0, 10, 12)
    shifts[2].wait_recv()
    send(2, 4, 0, 2, 1, 3)
    arrive(0, 4)
    owner(OWN, LEFT)
    arrive(1, 0, 2)
    send(1, 5, 6, 7, 8, 9, 11)
    arrive(0, 9, 10, 11, 12)
    owner(LEFT, OPP)
    arrive(1, 1, 3)
    send(1, 10, 12)
    arrive(1, 4)
    arrive(2, 4)
    expert_blocks(OWN, LEFT)
    arrive(0, 5, 6, 7, 8)
    send(0, 13, 14, 15, 16)
    arrive_small(0, 1)
    send_small(3, 4, 5)
    arrive(0, 13, 14, 15, 16)
    owner(OPP, 8)
    y_buf[...] = y_acc[...].astype(BF16)
    dx_buf[...] = dx_acc[...].astype(BF16)
    gate_exp[LEFT] = gate_columns(LEFT, expert)
    gate_exp[RIGHT] = gate_columns(RIGHT, expert)
    arrive_small(3, 4, 5)
    send_small(6)
    gate_exp[LEFT_SIB] = gate_columns(LEFT_SIB, expert)
    gate_exp[RIGHT_SIB] = gate_columns(RIGHT_SIB, expert)
    gate_exp[OPP] = gate_columns(OPP, expert)
    back = remote(dx_buf, dx_hbm, shift_send.at[3], shift_recv.at[3], before)
    back.start()
    started.append(back)
    y_out = pltpu.make_async_copy(y_buf, y_hbm, out_sem.at[0])
    y_out.start()
    arrive(2, 0, 2)
    send(2, 5, 6, 7, 8, 9, 11)
    arrive_small(6)
    gate_exp[OPP_SIB] = gate_columns(OPP_SIB, expert)
    arrive(2, 1, 3)
    send(2, 10, 12)
    arrive(1, 9, 10, 11, 12)
    arrive(2, 9, 10, 11, 12)
    expert_blocks(LEFT, OPP)
    arrive(1, 5, 6, 7, 8)
    send(1, 13, 14, 15, 16)
    arrive(1, 13, 14, 15, 16)
    for part in range(2):
        arrive(2, 5 + part, 7 + part)
        send(2, 13 + part, 15 + part)

        def near(step, carry):
            expert_rows(OPP, pl.ds(pl.multiple_of(step * half + part * quarter, quarter), quarter))
            return carry

        def far(step, carry):
            expert_rows(OPP_SIB, pl.ds(pl.multiple_of(step * half + part * quarter, quarter), quarter))
            return carry

        lax.fori_loop(0, 2, near, 0)
        arrive(2, 13 + part, 15 + part)
        lax.fori_loop(0, 2, far, 0)

    dup_ref[...] = dul_acc[:, :ff].astype(BF16)
    dlin_ref[...] = dul_acc[:, ff:].astype(BF16)
    ddown_ref[...] = ddown_acc[...].astype(BF16)
    for copy in started:
        copy.wait_send()
    back.wait_recv()
    y_out.wait()


def solution(mesh):
    stages = mesh.shape["stage"]
    groups = mesh.shape["expert"]
    tok_spec = P("stage", "expert", None)
    w_spec = P("stage", "expert", None, None)

    def device_step(x_act, route_idx, route_gate, w_up, w_lin, w_down, dy_out):
        _, tokens, d_model = x_act.shape
        ff = w_up.shape[-1]
        any_spec = pl.BlockSpec(memory_space=pl.ANY)
        vmem_spec = pl.BlockSpec(memory_space=pltpu.VMEM)
        dma = pltpu.SemaphoreType.DMA
        y_tok, dx_prev, g_up, g_lin, g_down = pl.pallas_call(
            functools.partial(moe_kernel, stages, groups),
            name="moe",
            out_shape=(
                jax.ShapeDtypeStruct((tokens, d_model), BF16),
                jax.ShapeDtypeStruct((tokens, d_model), BF16),
                jax.ShapeDtypeStruct((d_model, ff), BF16),
                jax.ShapeDtypeStruct((d_model, ff), BF16),
                jax.ShapeDtypeStruct((ff, d_model), BF16),
            ),
            in_specs=[any_spec] * 7,
            out_specs=(any_spec, any_spec, vmem_spec, vmem_spec, vmem_spec),
            scratch_shapes=[
                pltpu.VMEM((8, d_model + ff, d_model), BF16),
                pltpu.VMEM((8, tokens, d_model), BF16),
                pltpu.VMEM((8, tokens, d_model), BF16),
                pltpu.VMEM((8, 2, tokens), jnp.int32),
                pltpu.VMEM((8, 2, tokens), F32),
                pltpu.VMEM((8, tokens, 128), F32),
                pltpu.VMEM((8, tokens, 128), F32),
                pltpu.VMEM((tokens, d_model), F32),
                pltpu.VMEM((tokens, d_model), F32),
                pltpu.VMEM((tokens, d_model), BF16),
                pltpu.VMEM((tokens, d_model), BF16),
                pltpu.VMEM((d_model, 2 * ff), F32),
                pltpu.VMEM((ff, d_model), F32),
                dma((4,)),
                dma((3, 17)),
                dma((3, 17)),
                dma((2, 7)),
                dma((2, 7)),
                dma((4,)),
                dma((4,)),
                dma((1,)),
            ],
            compiler_params=pltpu.CompilerParams(collective_id=0, has_side_effects=True, vmem_limit_bytes=60 * 1024 * 1024),
        )(x_act[0], route_idx[0].T, route_gate[0].T, w_up[0, 0], w_lin[0, 0], w_down[0, 0], dy_out[0])
        return y_tok[None], dx_prev[None], g_up[None, None], g_lin[None, None], g_down[None, None]

    return jax.shard_map(device_step, mesh=mesh, in_specs=(tok_spec, tok_spec, tok_spec, w_spec, w_spec, w_spec, tok_spec), out_specs=(tok_spec, tok_spec, w_spec, w_spec, w_spec), check_vma=False)
```

```python
import functools

import jax
import jax.numpy as jnp
from jax import lax
from jax.experimental import pallas as pl
from jax.experimental.pallas import tpu as pltpu
from jax.sharding import PartitionSpec as P

F32 = jnp.float32
BF16 = jnp.bfloat16
MESH = pl.DeviceIdType.MESH

OWN, SIB, LEFT, LEFT_SIB, RIGHT, RIGHT_SIB, OPP, OPP_SIB = range(8)


def cols(gate, width):
    return jnp.concatenate([gate] * (width // 128), axis=1)


def nt_dot(a, b):
    return lax.dot_general(a, b, (((1,), (1,)), ((), ())), preferred_element_type=F32)


def tn_dot(a, b):
    return lax.dot_general(a, b, (((0,), (0,)), ((), ())), preferred_element_type=F32)


def nn_dot(a, b):
    return jnp.dot(a, b, preferred_element_type=F32)


def expert_math(x_rows, dy_rows, gate, w_ul, w_down):
    ff = w_down.shape[0]
    routed = cols(gate, ff) > 0.0
    pre = nn_dot(x_rows, w_ul)
    pre_up = jnp.where(routed, pre[:, :ff], 0.0)
    pre_lin = jnp.where(routed, pre[:, ff:], 0.0)
    sig = 1.0 / (1.0 + jnp.exp(-pre_up))
    act = pre_up * sig
    hidden = (act * pre_lin).astype(BF16)
    u_rows = (cols(gate, dy_rows.shape[1]) * dy_rows.astype(F32)).astype(BF16)
    d_hid = nt_dot(u_rows, w_down).astype(BF16).astype(F32)
    d_up = (d_hid * pre_lin * sig * (1.0 + pre_up * (1.0 - sig))).astype(BF16)
    d_lin = (d_hid * act).astype(BF16)
    return hidden, u_rows, jnp.concatenate([d_up, d_lin], axis=1)


def moe_kernel(
    stages, groups, x_hbm, idx_hbm, gate_hbm, up_hbm, lin_hbm, down_hbm, dy_hbm,
    y_ref, dx_ref, dup_ref, dlin_ref, ddown_ref,
    w_all, d_all, x_all, idx_all, gate_all, gate_own, gate_exp, y_acc, dx_acc, dx_buf, dul_acc, ddown_acc,
    load_sem, send_sem, recv_sem, small_send, small_recv, shift_send, shift_recv,
):
    tokens, d_model = x_hbm.shape
    ff = down_hbm.shape[0]
    half, cut = tokens // 2, 3 * tokens // 8
    rest = half - cut
    stage, expert = lax.axis_index("stage"), lax.axis_index("expert")
    core = lax.rem(expert, 2)
    right = {"expert": lax.rem(expert + 2, groups)}
    left = {"expert": lax.rem(expert + groups - 2, groups)}
    sib = {"expert": expert + 1 - 2 * core}
    after = {"stage": lax.rem(stage + 1, stages)}
    before = {"stage": lax.rem(stage + stages - 1, stages)}

    loads = [
        pltpu.make_async_copy(up_hbm, w_all.at[OWN, pl.ds(0, d_model), pl.ds(0, ff)], load_sem.at[0]),
        pltpu.make_async_copy(lin_hbm, w_all.at[OWN, pl.ds(0, d_model), pl.ds(ff, ff)], load_sem.at[1]),
        pltpu.make_async_copy(down_hbm, w_all.at[OWN, pl.ds(d_model, ff)], load_sem.at[2]),
        pltpu.make_async_copy(dy_hbm, d_all.at[OWN], load_sem.at[3]),
    ]
    for load in loads:
        load.start()

    barrier = pltpu.get_barrier_semaphore()
    for peer in (right, left, sib, after, before):
        pl.semaphore_signal(barrier, inc=1, device_id=peer, device_id_type=MESH)
    pl.semaphore_wait(barrier, 5)

    started = []

    def remote(src, dst, send, recv, peer):
        return pltpu.make_async_remote_copy(src_ref=src, dst_ref=dst, send_sem=send, recv_sem=recv, device_id=peer, device_id_type=MESH)

    arrays = (w_all, d_all, x_all)
    kinds = [
        (OWN, LEFT, 0, half, right), (OWN, LEFT, half, half, right),
        (OWN, RIGHT, half, half, left), (OWN, RIGHT, 0, half, left),
        (OWN, SIB, 0, tokens, sib),
        (LEFT, OPP, 0, cut, right), (LEFT, OPP, cut, rest, right),
        (RIGHT, OPP, tokens - cut, cut, left), (RIGHT, OPP, half, rest, left),
        (LEFT, LEFT_SIB, 0, half, sib), (LEFT, LEFT_SIB, half, half, sib),
        (RIGHT, RIGHT_SIB, half, half, sib), (RIGHT, RIGHT_SIB, 0, half, sib),
        (OPP, OPP_SIB, 0, cut, sib), (OPP, OPP_SIB, cut, rest, sib),
        (OPP, OPP_SIB, tokens - cut, cut, sib), (OPP, OPP_SIB, half, rest, sib),
    ]

    def block_copy(array, kind):
        src_slot, dst_slot, row, rows, peer = kinds[kind]
        ref = arrays[array]
        return remote(
            ref.at[src_slot, pl.ds(row, rows)], ref.at[dst_slot, pl.ds(row, rows)],
            send_sem.at[array, kind], recv_sem.at[array, kind], peer,
        )

    def send(array, *which):
        for kind in which:
            copy = block_copy(array, kind)
            copy.start()
            started.append(copy)

    def arrive(array, *which):
        for kind in which:
            block_copy(array, kind).wait_recv()

    small = [(OWN, LEFT, right), (OWN, RIGHT, left), (OWN, SIB, sib), (LEFT, OPP, right), (LEFT, LEFT_SIB, sib), (RIGHT, RIGHT_SIB, sib), (OPP, OPP_SIB, sib)]

    def small_copies(kind):
        src_slot, dst_slot, peer = small[kind]
        return [
            remote(ref.at[src_slot], ref.at[dst_slot], small_send.at[which, kind], small_recv.at[which, kind], peer)
            for which, ref in enumerate((idx_all, gate_all))
        ]

    def send_small(*which):
        for kind in which:
            for copy in small_copies(kind):
                copy.start()
                started.append(copy)

    def arrive_small(*which):
        for kind in which:
            for copy in small_copies(kind):
                copy.wait_recv()

    shifts = [
        remote(idx_hbm, idx_all.at[OWN], shift_send.at[0], shift_recv.at[0], after),
        remote(gate_hbm, gate_all.at[OWN], shift_send.at[1], shift_recv.at[1], after),
        remote(x_hbm, x_all.at[OWN], shift_send.at[2], shift_recv.at[2], after),
    ]
    for copy in shifts:
        copy.start()
        started.append(copy)
    for load in loads:
        load.wait()
    send(0, 0, 2, 1, 3, 4)

    def gate_columns(slot, expert_id):
        ids, gates = idx_all[slot], gate_all[slot]
        row = jnp.sum(jnp.where(ids == expert_id, gates, 0.0), axis=0, keepdims=True)
        return jnp.broadcast_to(row, (128, tokens)).T

    def expert_at(slot):
        chip_step = (0, 0, groups - 2, groups - 2, 2, 2, 4, 4)[slot]
        flip = (1 - 2 * core) if slot % 2 else 0
        return lax.rem(expert + flip + chip_step, groups)

    shifts[0].wait_recv()
    shifts[1].wait_recv()
    send_small(2, 0, 1)
    send(1, 0, 2, 1, 3, 4)
    for slot in range(8):
        gate_own[slot] = gate_columns(OWN, expert_at(slot))
    gate_exp[OWN] = gate_columns(OWN, expert)
    y_acc[...] = jnp.zeros_like(y_acc)
    dx_acc[...] = jnp.zeros_like(dx_acc)
    dul_acc[...] = jnp.zeros_like(dul_acc)
    ddown_acc[...] = jnp.zeros_like(ddown_acc)
    arrive_small(2)
    gate_exp[SIB] = gate_columns(SIB, expert)

    def owner(first, last):
        def body(step, carry):
            slot = first + step // 2
            rows = pl.ds(pl.multiple_of(lax.rem(step, 2) * half, half), half)
            w_ul, w_down = w_all[slot, pl.ds(0, d_model)], w_all[slot, pl.ds(d_model, ff)]
            gate = gate_own[slot, rows]
            hidden, _, d_ul = expert_math(x_all[OWN, rows], d_all[OWN, rows], gate, w_ul, w_down)
            out = nn_dot(hidden, w_down).astype(BF16).astype(F32)
            y_acc[rows] += cols(gate, d_model) * out
            dx_acc[rows] += nt_dot(d_ul, w_ul).astype(BF16).astype(F32)
            return carry

        lax.fori_loop(0, 2 * (last - first), body, 0)

    def expert_rows(slot, rows):
        w_ul, w_down = w_all[OWN, pl.ds(0, d_model)], w_all[OWN, pl.ds(d_model, ff)]
        x_rows = x_all[slot, rows]
        hidden, u_rows, d_ul = expert_math(x_rows, d_all[slot, rows], gate_exp[slot, rows], w_ul, w_down)
        dul_acc[...] += tn_dot(x_rows, d_ul)
        ddown_acc[...] += tn_dot(hidden, u_rows)

    def expert_blocks(first, last):
        def body(step, carry):
            expert_rows(first + step // 2, pl.ds(pl.multiple_of(lax.rem(step, 2) * half, half), half))
            return carry

        lax.fori_loop(0, 2 * (last - first), body, 0)

    arrive(0, 0, 2)
    send(0, 5, 6, 7, 8, 9, 11)
    arrive_small(0, 1)
    send_small(3, 4, 5)
    gate_exp[LEFT] = gate_columns(LEFT, expert)
    gate_exp[RIGHT] = gate_columns(RIGHT, expert)
    arrive(0, 1, 3)
    send(0, 10, 12)
    shifts[2].wait_recv()
    send(2, 4, 0, 2, 1, 3)
    arrive(0, 4)
    owner(OWN, LEFT)
    arrive(1, 0, 2)
    send(1, 5, 6, 7, 8, 9, 11)
    arrive(0, 9, 10, 11, 12)
    owner(LEFT, OPP)
    arrive(1, 1, 3)
    send(1, 10, 12)
    arrive_small(3, 4, 5)
    send_small(6)
    gate_exp[LEFT_SIB] = gate_columns(LEFT_SIB, expert)
    gate_exp[RIGHT_SIB] = gate_columns(RIGHT_SIB, expert)
    gate_exp[OPP] = gate_columns(OPP, expert)
    arrive(1, 4)
    arrive(2, 4)
    expert_blocks(OWN, LEFT)
    arrive(0, 5, 6, 7, 8)
    send(0, 13, 14, 15, 16)
    arrive_small(6)
    gate_exp[OPP_SIB] = gate_columns(OPP_SIB, expert)
    arrive(0, 13, 14, 15, 16)
    owner(OPP, 8)
    y_ref[...] = y_acc[...].astype(BF16)
    dx_buf[...] = dx_acc[...].astype(BF16)
    arrive(2, 0, 2)
    send(2, 5, 6, 7, 8, 9, 11)
    back = remote(dx_buf, dx_ref, shift_send.at[3], shift_recv.at[3], before)
    back.start()
    started.append(back)
    arrive(2, 1, 3)
    send(2, 10, 12)
    arrive(1, 9, 10, 11, 12)
    arrive(2, 9, 10, 11, 12)
    expert_blocks(LEFT, OPP)
    arrive(1, 5, 6, 7, 8)
    send(1, 13, 14, 15, 16)
    arrive(2, 5, 7)
    send(2, 13, 15)

    def outer(slot):
        def body(step, carry):
            expert_rows(slot, pl.ds(pl.multiple_of(step * (tokens - cut), 32), cut))
            return carry

        lax.fori_loop(0, 2, body, 0)

    outer(OPP)
    arrive(1, 13, 14, 15, 16)
    arrive(2, 13, 15)
    outer(OPP_SIB)
    arrive(2, 6, 8)
    send(2, 14, 16)
    expert_rows(OPP, pl.ds(cut, 2 * rest))
    arrive(2, 14, 16)
    expert_rows(OPP_SIB, pl.ds(cut, 2 * rest))

    dup_ref[...] = dul_acc[:, :ff].astype(BF16)
    dlin_ref[...] = dul_acc[:, ff:].astype(BF16)
    ddown_ref[...] = ddown_acc[...].astype(BF16)
    for copy in started:
        copy.wait_send()
    back.wait_recv()


def finish_kernel(*refs):
    count = len(refs) // 2
    outs = [pltpu.make_async_copy(refs[i], refs[count + i], refs[-1].at[i]) for i in range(count)]
    for copy in outs:
        copy.start()
    for copy in outs:
        copy.wait()


def solution(mesh):
    stages = mesh.shape["stage"]
    groups = mesh.shape["expert"]
    tok_spec = P("stage", "expert", None)
    w_spec = P("stage", "expert", None, None)

    def device_step(x_act, route_idx, route_gate, w_up, w_lin, w_down, dy_out):
        _, tokens, d_model = x_act.shape
        ff = w_up.shape[-1]
        any_spec = pl.BlockSpec(memory_space=pl.ANY)
        vmem_spec = pl.BlockSpec(memory_space=pltpu.VMEM)
        dma = pltpu.SemaphoreType.DMA
        results = pl.pallas_call(
            functools.partial(moe_kernel, stages, groups),
            name="moe",
            out_shape=(
                pltpu.VMEM((tokens, d_model), BF16),
                pltpu.VMEM((tokens, d_model), BF16),
                pltpu.VMEM((d_model, ff), BF16),
                pltpu.VMEM((d_model, ff), BF16),
                pltpu.VMEM((ff, d_model), BF16),
            ),
            in_specs=[any_spec] * 7,
            out_specs=(vmem_spec,) * 5,
            scratch_shapes=[
                pltpu.VMEM((8, d_model + ff, d_model), BF16),
                pltpu.VMEM((8, tokens, d_model), BF16),
                pltpu.VMEM((8, tokens, d_model), BF16),
                pltpu.VMEM((8, 2, tokens), jnp.int32),
                pltpu.VMEM((8, 2, tokens), F32),
                pltpu.VMEM((8, tokens, 128), F32),
                pltpu.VMEM((8, tokens, 128), F32),
                pltpu.VMEM((tokens, d_model), F32),
                pltpu.VMEM((tokens, d_model), F32),
                pltpu.VMEM((tokens, d_model), BF16),
                pltpu.VMEM((d_model, 2 * ff), F32),
                pltpu.VMEM((ff, d_model), F32),
                dma((4,)),
                dma((3, 17)),
                dma((3, 17)),
                dma((2, 7)),
                dma((2, 7)),
                dma((4,)),
                dma((4,)),
            ],
            compiler_params=pltpu.CompilerParams(collective_id=0, has_side_effects=True, vmem_limit_bytes=60 * 1024 * 1024),
        )(x_act[0], route_idx[0].T, route_gate[0].T, w_up[0, 0], w_lin[0, 0], w_down[0, 0], dy_out[0])
        shapes = [jax.ShapeDtypeStruct(r.shape, r.dtype) for r in results]
        y_tok, dx_prev, g_up, g_lin, g_down = pl.pallas_call(
            finish_kernel,
            name="finish",
            out_shape=shapes,
            in_specs=[vmem_spec] * 5,
            out_specs=[any_spec] * 5,
            scratch_shapes=[dma((5,))],
        )(*[pltpu.with_memory_space_constraint(r, pltpu.VMEM) for r in results])
        return y_tok[None], dx_prev[None], g_up[None, None], g_lin[None, None], g_down[None, None]

    return jax.shard_map(device_step, mesh=mesh, in_specs=(tok_spec, tok_spec, tok_spec, w_spec, w_spec, w_spec, tok_spec), out_specs=(tok_spec, tok_spec, w_spec, w_spec, w_spec), check_vma=False)
```

```python
import functools

import jax
import jax.numpy as jnp
from jax import lax
from jax.experimental import pallas as pl
from jax.experimental.pallas import tpu as pltpu
from jax.sharding import PartitionSpec as P

F32 = jnp.float32
BF16 = jnp.bfloat16
MESH = pl.DeviceIdType.MESH

OWN, SIB, LEFT, LEFT_SIB, RIGHT, RIGHT_SIB, OPP, OPP_SIB = range(8)


def cols(gate, width):
    return jnp.concatenate([gate] * (width // 128), axis=1)


def nt_dot(a, b):
    return lax.dot_general(a, b, (((1,), (1,)), ((), ())), preferred_element_type=F32)


def tn_dot(a, b):
    return lax.dot_general(a, b, (((0,), (0,)), ((), ())), preferred_element_type=F32)


def nn_dot(a, b):
    return jnp.dot(a, b, preferred_element_type=F32)


def expert_math(x_rows, dy_rows, gate, w_ul, w_down):
    ff = w_down.shape[0]
    routed = cols(gate, ff) > 0.0
    pre = nn_dot(x_rows, w_ul)
    pre_up = jnp.where(routed, pre[:, :ff], 0.0)
    pre_lin = jnp.where(routed, pre[:, ff:], 0.0)
    sig = 1.0 / (1.0 + jnp.exp(-pre_up))
    act = pre_up * sig
    hidden = (act * pre_lin).astype(BF16)
    u_rows = (cols(gate, dy_rows.shape[1]) * dy_rows.astype(F32)).astype(BF16)
    d_hid = nt_dot(u_rows, w_down).astype(BF16).astype(F32)
    d_up = (d_hid * pre_lin * sig * (1.0 + pre_up * (1.0 - sig))).astype(BF16)
    d_lin = (d_hid * act).astype(BF16)
    return hidden, u_rows, jnp.concatenate([d_up, d_lin], axis=1)


def moe_kernel(
    stages, groups, x_hbm, idx_hbm, gate_hbm, up_hbm, lin_hbm, down_hbm, dy_hbm,
    y_ref, dx_ref, dup_ref, dlin_ref, ddown_ref,
    w_all, d_all, x_all, idx_all, gate_all, gate_own, gate_exp, y_acc, dx_acc, dx_buf, dul_acc, ddown_acc,
    load_sem, send_sem, recv_sem, small_send, small_recv, shift_send, shift_recv, ring_ready, stage_ready, sib_ready,
):
    tokens, d_model = x_hbm.shape
    ff = down_hbm.shape[0]
    half, cut = tokens // 2, 3 * tokens // 8
    rest = half - cut
    stage, expert = lax.axis_index("stage"), lax.axis_index("expert")
    core = lax.rem(expert, 2)
    right = {"expert": lax.rem(expert + 2, groups)}
    left = {"expert": lax.rem(expert + groups - 2, groups)}
    sib = {"expert": expert + 1 - 2 * core}
    after = {"stage": lax.rem(stage + 1, stages)}
    before = {"stage": lax.rem(stage + stages - 1, stages)}

    loads = [
        pltpu.make_async_copy(up_hbm, w_all.at[OWN, pl.ds(0, d_model), pl.ds(0, ff)], load_sem.at[0]),
        pltpu.make_async_copy(lin_hbm, w_all.at[OWN, pl.ds(0, d_model), pl.ds(ff, ff)], load_sem.at[1]),
        pltpu.make_async_copy(down_hbm, w_all.at[OWN, pl.ds(d_model, ff)], load_sem.at[2]),
        pltpu.make_async_copy(dy_hbm, d_all.at[OWN], load_sem.at[3]),
    ]
    for load in loads:
        load.start()

    barrier = pltpu.get_barrier_semaphore()
    colour = lax.rem(expert // 2 + core, 2)

    def signal(sem, *peers):
        for peer in peers:
            pl.semaphore_signal(sem, inc=1, device_id=peer, device_id_type=MESH)

    @pl.when(colour == 1)
    def _():
        signal(barrier, right, left, sib, after, before)

    @pl.when(colour == 0)
    def _():
        pl.semaphore_wait(barrier, 3)
        signal(ring_ready, right, left, sib)

    @pl.when(colour == 1)
    def _():
        pl.semaphore_wait(ring_ready, 3)

    started = []

    def remote(src, dst, send, recv, peer):
        return pltpu.make_async_remote_copy(src_ref=src, dst_ref=dst, send_sem=send, recv_sem=recv, device_id=peer, device_id_type=MESH)

    arrays = (w_all, d_all, x_all)
    kinds = [
        (OWN, LEFT, 0, half, right), (OWN, LEFT, half, half, right),
        (OWN, RIGHT, half, half, left), (OWN, RIGHT, 0, half, left),
        (OWN, SIB, 0, tokens, sib),
        (LEFT, OPP, 0, cut, right), (LEFT, OPP, cut, rest, right),
        (RIGHT, OPP, tokens - cut, cut, left), (RIGHT, OPP, half, rest, left),
        (LEFT, LEFT_SIB, 0, half, sib), (LEFT, LEFT_SIB, half, half, sib),
        (RIGHT, RIGHT_SIB, half, half, sib), (RIGHT, RIGHT_SIB, 0, half, sib),
        (OPP, OPP_SIB, 0, cut, sib), (OPP, OPP_SIB, cut, rest, sib),
        (OPP, OPP_SIB, tokens - cut, cut, sib), (OPP, OPP_SIB, half, rest, sib),
    ]

    def block_copy(array, kind):
        src_slot, dst_slot, row, rows, peer = kinds[kind]
        ref = arrays[array]
        return remote(
            ref.at[src_slot, pl.ds(row, rows)], ref.at[dst_slot, pl.ds(row, rows)],
            send_sem.at[array, kind], recv_sem.at[array, kind], peer,
        )

    def send(array, *which):
        for kind in which:
            copy = block_copy(array, kind)
            copy.start()
            started.append(copy)

    def arrive(array, *which):
        for kind in which:
            block_copy(array, kind).wait_recv()

    small = [(OWN, LEFT, right), (OWN, RIGHT, left), (OWN, SIB, sib), (LEFT, OPP, right), (LEFT, LEFT_SIB, sib), (RIGHT, RIGHT_SIB, sib), (OPP, OPP_SIB, sib)]

    def small_copies(kind):
        src_slot, dst_slot, peer = small[kind]
        return [
            remote(ref.at[src_slot], ref.at[dst_slot], small_send.at[which, kind], small_recv.at[which, kind], peer)
            for which, ref in enumerate((idx_all, gate_all))
        ]

    def send_small(*which):
        for kind in which:
            for copy in small_copies(kind):
                copy.start()
                started.append(copy)

    def arrive_small(*which):
        for kind in which:
            for copy in small_copies(kind):
                copy.wait_recv()

    for load in loads:
        load.wait()
    send(0, 0, 2, 1, 3, 4)

    @pl.when(colour == 1)
    def _():
        pl.semaphore_wait(barrier, 2)
        signal(stage_ready, after, before)
        pl.semaphore_wait(stage_ready, 2)
        signal(sib_ready, sib)

    @pl.when(colour == 0)
    def _():
        pl.semaphore_wait(sib_ready, 1)

    shifts = [
        remote(idx_hbm, idx_all.at[OWN], shift_send.at[0], shift_recv.at[0], after),
        remote(gate_hbm, gate_all.at[OWN], shift_send.at[1], shift_recv.at[1], after),
        remote(x_hbm, x_all.at[OWN], shift_send.at[2], shift_recv.at[2], after),
    ]
    for copy in shifts:
        copy.start()
        started.append(copy)

    def gate_columns(slot, expert_id):
        ids, gates = idx_all[slot], gate_all[slot]
        row = jnp.sum(jnp.where(ids == expert_id, gates, 0.0), axis=0, keepdims=True)
        return jnp.broadcast_to(row, (128, tokens)).T

    def expert_at(slot):
        chip_step = (0, 0, groups - 2, groups - 2, 2, 2, 4, 4)[slot]
        flip = (1 - 2 * core) if slot % 2 else 0
        return lax.rem(expert + flip + chip_step, groups)

    shifts[0].wait_recv()
    shifts[1].wait_recv()
    send_small(2, 0, 1)
    send(1, 0, 2, 1, 3, 4)
    for slot in range(8):
        gate_own[slot] = gate_columns(OWN, expert_at(slot))
    gate_exp[OWN] = gate_columns(OWN, expert)
    y_acc[...] = jnp.zeros_like(y_acc)
    dx_acc[...] = jnp.zeros_like(dx_acc)
    dul_acc[...] = jnp.zeros_like(dul_acc)
    ddown_acc[...] = jnp.zeros_like(ddown_acc)
    arrive_small(2)
    gate_exp[SIB] = gate_columns(SIB, expert)

    def owner(first, last):
        def body(step, carry):
            slot = first + step // 2
            rows = pl.ds(pl.multiple_of(lax.rem(step, 2) * half, half), half)
            w_ul, w_down = w_all[slot, pl.ds(0, d_model)], w_all[slot, pl.ds(d_model, ff)]
            gate = gate_own[slot, rows]
            hidden, _, d_ul = expert_math(x_all[OWN, rows], d_all[OWN, rows], gate, w_ul, w_down)
            out = nn_dot(hidden, w_down).astype(BF16).astype(F32)
            y_acc[rows] += cols(gate, d_model) * out
            dx_acc[rows] += nt_dot(d_ul, w_ul).astype(BF16).astype(F32)
            return carry

        lax.fori_loop(0, 2 * (last - first), body, 0)

    def expert_rows(slot, rows):
        w_ul, w_down = w_all[OWN, pl.ds(0, d_model)], w_all[OWN, pl.ds(d_model, ff)]
        x_rows = x_all[slot, rows]
        hidden, u_rows, d_ul = expert_math(x_rows, d_all[slot, rows], gate_exp[slot, rows], w_ul, w_down)
        dul_acc[...] += tn_dot(x_rows, d_ul)
        ddown_acc[...] += tn_dot(hidden, u_rows)

    def expert_blocks(first, last):
        def body(step, carry):
            expert_rows(first + step // 2, pl.ds(pl.multiple_of(lax.rem(step, 2) * half, half), half))
            return carry

        lax.fori_loop(0, 2 * (last - first), body, 0)

    arrive(0, 0, 2)
    send(0, 5, 6, 7, 8, 9, 11)
    arrive_small(0, 1)
    send_small(3, 4, 5)
    gate_exp[LEFT] = gate_columns(LEFT, expert)
    gate_exp[RIGHT] = gate_columns(RIGHT, expert)
    arrive(0, 1, 3)
    send(0, 10, 12)
    shifts[2].wait_recv()
    send(2, 4, 0, 2, 1, 3)
    arrive(0, 4)
    owner(OWN, LEFT)
    arrive(1, 0, 2)
    send(1, 5, 6, 7, 8, 9, 11)
    arrive(0, 9, 10, 11, 12)
    owner(LEFT, OPP)
    arrive(1, 1, 3)
    send(1, 10, 12)
    arrive_small(3, 4, 5)
    send_small(6)
    gate_exp[LEFT_SIB] = gate_columns(LEFT_SIB, expert)
    gate_exp[RIGHT_SIB] = gate_columns(RIGHT_SIB, expert)
    gate_exp[OPP] = gate_columns(OPP, expert)
    arrive(1, 4)
    arrive(2, 4)
    expert_blocks(OWN, LEFT)
    arrive(0, 5, 6, 7, 8)
    send(0, 13, 14, 15, 16)
    arrive_small(6)
    gate_exp[OPP_SIB] = gate_columns(OPP_SIB, expert)
    arrive(0, 13, 14, 15, 16)
    owner(OPP, 8)
    y_ref[...] = y_acc[...].astype(BF16)
    dx_buf[...] = dx_acc[...].astype(BF16)
    arrive(2, 0, 2)
    send(2, 5, 6, 7, 8, 9, 11)
    back = remote(dx_buf, dx_ref, shift_send.at[3], shift_recv.at[3], before)
    back.start()
    started.append(back)
    arrive(2, 1, 3)
    send(2, 10, 12)
    arrive(1, 9, 10, 11, 12)
    arrive(2, 9, 10, 11, 12)
    expert_blocks(LEFT, OPP)
    arrive(1, 5, 6, 7, 8)
    send(1, 13, 14, 15, 16)
    arrive(2, 5, 7)
    send(2, 13, 15)

    def outer(slot):
        def body(step, carry):
            expert_rows(slot, pl.ds(pl.multiple_of(step * (tokens - cut), 32), cut))
            return carry

        lax.fori_loop(0, 2, body, 0)

    outer(OPP)
    arrive(1, 13, 14, 15, 16)
    arrive(2, 13, 15)
    outer(OPP_SIB)
    arrive(2, 6, 8)
    send(2, 14, 16)
    expert_rows(OPP, pl.ds(cut, 2 * rest))
    arrive(2, 14, 16)
    expert_rows(OPP_SIB, pl.ds(cut, 2 * rest))

    dup_ref[...] = dul_acc[:, :ff].astype(BF16)
    dlin_ref[...] = dul_acc[:, ff:].astype(BF16)
    ddown_ref[...] = ddown_acc[...].astype(BF16)
    for copy in started:
        copy.wait_send()
    back.wait_recv()


def finish_kernel(*refs):
    count = len(refs) // 2
    outs = [pltpu.make_async_copy(refs[i], refs[count + i], refs[-1].at[i]) for i in range(count)]
    for copy in outs:
        copy.start()
    for copy in outs:
        copy.wait()


def solution(mesh):
    stages = mesh.shape["stage"]
    groups = mesh.shape["expert"]
    tok_spec = P("stage", "expert", None)
    w_spec = P("stage", "expert", None, None)

    def device_step(x_act, route_idx, route_gate, w_up, w_lin, w_down, dy_out):
        _, tokens, d_model = x_act.shape
        ff = w_up.shape[-1]
        any_spec = pl.BlockSpec(memory_space=pl.ANY)
        vmem_spec = pl.BlockSpec(memory_space=pltpu.VMEM)
        dma = pltpu.SemaphoreType.DMA
        results = pl.pallas_call(
            functools.partial(moe_kernel, stages, groups),
            name="moe",
            out_shape=(
                pltpu.VMEM((tokens, d_model), BF16),
                pltpu.VMEM((tokens, d_model), BF16),
                pltpu.VMEM((d_model, ff), BF16),
                pltpu.VMEM((d_model, ff), BF16),
                pltpu.VMEM((ff, d_model), BF16),
            ),
            in_specs=[any_spec] * 7,
            out_specs=(vmem_spec,) * 5,
            scratch_shapes=[
                pltpu.VMEM((8, d_model + ff, d_model), BF16),
                pltpu.VMEM((8, tokens, d_model), BF16),
                pltpu.VMEM((8, tokens, d_model), BF16),
                pltpu.VMEM((8, 2, tokens), jnp.int32),
                pltpu.VMEM((8, 2, tokens), F32),
                pltpu.VMEM((8, tokens, 128), F32),
                pltpu.VMEM((8, tokens, 128), F32),
                pltpu.VMEM((tokens, d_model), F32),
                pltpu.VMEM((tokens, d_model), F32),
                pltpu.VMEM((tokens, d_model), BF16),
                pltpu.VMEM((d_model, 2 * ff), F32),
                pltpu.VMEM((ff, d_model), F32),
                dma((4,)),
                dma((3, 17)),
                dma((3, 17)),
                dma((2, 7)),
                dma((2, 7)),
                dma((4,)),
                dma((4,)),
                pltpu.SemaphoreType.REGULAR,
                pltpu.SemaphoreType.REGULAR,
                pltpu.SemaphoreType.REGULAR,
            ],
            compiler_params=pltpu.CompilerParams(collective_id=0, has_side_effects=True, vmem_limit_bytes=60 * 1024 * 1024),
        )(x_act[0], route_idx[0].T, route_gate[0].T, w_up[0, 0], w_lin[0, 0], w_down[0, 0], dy_out[0])
        shapes = [jax.ShapeDtypeStruct(r.shape, r.dtype) for r in results]
        y_tok, dx_prev, g_up, g_lin, g_down = pl.pallas_call(
            finish_kernel,
            name="finish",
            out_shape=shapes,
            in_specs=[vmem_spec] * 5,
            out_specs=[any_spec] * 5,
            scratch_shapes=[dma((5,))],
        )(*[pltpu.with_memory_space_constraint(r, pltpu.VMEM) for r in results])
        return y_tok[None], dx_prev[None], g_up[None, None], g_lin[None, None], g_down[None, None]

    return jax.shard_map(device_step, mesh=mesh, in_specs=(tok_spec, tok_spec, tok_spec, w_spec, w_spec, w_spec, tok_spec), out_specs=(tok_spec, tok_spec, w_spec, w_spec, w_spec), check_vma=False)
```

```python
import functools

import jax
import jax.numpy as jnp
from jax import lax
from jax.experimental import pallas as pl
from jax.experimental.pallas import tpu as pltpu
from jax.sharding import PartitionSpec as P

F32 = jnp.float32
BF16 = jnp.bfloat16
MESH = pl.DeviceIdType.MESH

OWN, SIB, LEFT, LEFT_SIB, RIGHT, RIGHT_SIB, OPP, OPP_SIB = range(8)


def cols(gate, width):
    return jnp.concatenate([gate] * (width // 128), axis=1)


def nt_dot(a, b):
    return lax.dot_general(a, b, (((1,), (1,)), ((), ())), preferred_element_type=F32)


def tn_dot(a, b):
    return lax.dot_general(a, b, (((0,), (0,)), ((), ())), preferred_element_type=F32)


def nn_dot(a, b):
    return jnp.dot(a, b, preferred_element_type=F32)


def hidden_cotangent(dy_rows, gate, w_down):
    u_rows = (cols(gate, dy_rows.shape[1]) * dy_rows.astype(F32)).astype(BF16)
    return u_rows, nt_dot(u_rows, w_down).astype(BF16)


def expert_math(x_rows, dy_rows, gate, w_ul, w_down, ready=None):
    ff = w_down.shape[0]
    routed = cols(gate, ff) > 0.0
    pre = nn_dot(x_rows, w_ul)
    pre_up = jnp.where(routed, pre[:, :ff], 0.0)
    pre_lin = jnp.where(routed, pre[:, ff:], 0.0)
    sig = 1.0 / (1.0 + jnp.exp(-pre_up))
    act = pre_up * sig
    hidden = (act * pre_lin).astype(BF16)
    u_rows, d_hid = hidden_cotangent(dy_rows, gate, w_down) if ready is None else ready
    d_hid = d_hid.astype(F32)
    d_up = (d_hid * pre_lin * sig * (1.0 + pre_up * (1.0 - sig))).astype(BF16)
    d_lin = (d_hid * act).astype(BF16)
    return hidden, u_rows, jnp.concatenate([d_up, d_lin], axis=1)


def moe_kernel(
    stages, groups, x_hbm, idx_hbm, gate_hbm, up_hbm, lin_hbm, down_hbm, dy_hbm,
    y_ref, dx_ref, dup_ref, dlin_ref, ddown_ref,
    w_all, d_all, x_all, idx_all, gate_all, gate_own, gate_exp, y_acc, dx_acc, dx_buf, dul_acc, ddown_acc, u_opp, dh_opp,
    load_sem, send_sem, recv_sem, small_send, small_recv, shift_send, shift_recv, ring_ready, stage_ready, sib_ready,
):
    tokens, d_model = x_hbm.shape
    ff = down_hbm.shape[0]
    half, cut = tokens // 2, 3 * tokens // 8
    rest = half - cut
    stage, expert = lax.axis_index("stage"), lax.axis_index("expert")
    core = lax.rem(expert, 2)
    right = {"expert": lax.rem(expert + 2, groups)}
    left = {"expert": lax.rem(expert + groups - 2, groups)}
    sib = {"expert": expert + 1 - 2 * core}
    after = {"stage": lax.rem(stage + 1, stages)}
    before = {"stage": lax.rem(stage + stages - 1, stages)}

    loads = [
        pltpu.make_async_copy(up_hbm, w_all.at[OWN, pl.ds(0, d_model), pl.ds(0, ff)], load_sem.at[0]),
        pltpu.make_async_copy(lin_hbm, w_all.at[OWN, pl.ds(0, d_model), pl.ds(ff, ff)], load_sem.at[1]),
        pltpu.make_async_copy(down_hbm, w_all.at[OWN, pl.ds(d_model, ff)], load_sem.at[2]),
        pltpu.make_async_copy(dy_hbm, d_all.at[OWN], load_sem.at[3]),
    ]
    for load in loads:
        load.start()

    barrier = pltpu.get_barrier_semaphore()
    colour = lax.rem(expert // 2 + core, 2)

    def signal(sem, *peers):
        for peer in peers:
            pl.semaphore_signal(sem, inc=1, device_id=peer, device_id_type=MESH)

    @pl.when(colour == 1)
    def _():
        signal(barrier, right, left, sib, after, before)

    @pl.when(colour == 0)
    def _():
        pl.semaphore_wait(barrier, 3)
        signal(ring_ready, right, left, sib)

    @pl.when(colour == 1)
    def _():
        pl.semaphore_wait(ring_ready, 3)

    started = []

    def remote(src, dst, send, recv, peer):
        return pltpu.make_async_remote_copy(src_ref=src, dst_ref=dst, send_sem=send, recv_sem=recv, device_id=peer, device_id_type=MESH)

    arrays = (w_all, d_all, x_all)
    kinds = [
        (OWN, LEFT, 0, half, right), (OWN, LEFT, half, half, right),
        (OWN, RIGHT, half, half, left), (OWN, RIGHT, 0, half, left),
        (OWN, SIB, 0, tokens, sib),
        (LEFT, OPP, 0, cut, right), (LEFT, OPP, cut, rest, right),
        (RIGHT, OPP, tokens - cut, cut, left), (RIGHT, OPP, half, rest, left),
        (LEFT, LEFT_SIB, 0, half, sib), (LEFT, LEFT_SIB, half, half, sib),
        (RIGHT, RIGHT_SIB, half, half, sib), (RIGHT, RIGHT_SIB, 0, half, sib),
        (OPP, OPP_SIB, 0, cut, sib), (OPP, OPP_SIB, cut, rest, sib),
        (OPP, OPP_SIB, tokens - cut, cut, sib), (OPP, OPP_SIB, half, rest, sib),
    ]

    def block_copy(array, kind):
        src_slot, dst_slot, row, rows, peer = kinds[kind]
        ref = arrays[array]
        return remote(
            ref.at[src_slot, pl.ds(row, rows)], ref.at[dst_slot, pl.ds(row, rows)],
            send_sem.at[array, kind], recv_sem.at[array, kind], peer,
        )

    def send(array, *which):
        for kind in which:
            copy = block_copy(array, kind)
            copy.start()
            started.append(copy)

    def arrive(array, *which):
        for kind in which:
            block_copy(array, kind).wait_recv()

    small = [(OWN, LEFT, right), (OWN, RIGHT, left), (OWN, SIB, sib), (LEFT, OPP, right), (LEFT, LEFT_SIB, sib), (RIGHT, RIGHT_SIB, sib), (OPP, OPP_SIB, sib)]

    def small_copies(kind):
        src_slot, dst_slot, peer = small[kind]
        return [
            remote(ref.at[src_slot], ref.at[dst_slot], small_send.at[which, kind], small_recv.at[which, kind], peer)
            for which, ref in enumerate((idx_all, gate_all))
        ]

    def send_small(*which):
        for kind in which:
            for copy in small_copies(kind):
                copy.start()
                started.append(copy)

    def arrive_small(*which):
        for kind in which:
            for copy in small_copies(kind):
                copy.wait_recv()

    for load in loads:
        load.wait()
    send(0, 0, 2, 1, 3, 4)

    @pl.when(colour == 1)
    def _():
        pl.semaphore_wait(barrier, 2)
        signal(stage_ready, after, before)
        pl.semaphore_wait(stage_ready, 2)
        signal(sib_ready, sib)

    @pl.when(colour == 0)
    def _():
        pl.semaphore_wait(sib_ready, 1)

    shifts = [
        remote(idx_hbm, idx_all.at[OWN], shift_send.at[0], shift_recv.at[0], after),
        remote(gate_hbm, gate_all.at[OWN], shift_send.at[1], shift_recv.at[1], after),
        remote(x_hbm, x_all.at[OWN], shift_send.at[2], shift_recv.at[2], after),
    ]
    for copy in shifts:
        copy.start()
        started.append(copy)

    def gate_columns(slot, expert_id):
        ids, gates = idx_all[slot], gate_all[slot]
        row = jnp.sum(jnp.where(ids == expert_id, gates, 0.0), axis=0, keepdims=True)
        return jnp.broadcast_to(row, (128, tokens)).T

    def expert_at(slot):
        chip_step = (0, 0, groups - 2, groups - 2, 2, 2, 4, 4)[slot]
        flip = (1 - 2 * core) if slot % 2 else 0
        return lax.rem(expert + flip + chip_step, groups)

    shifts[0].wait_recv()
    shifts[1].wait_recv()
    send_small(2, 0, 1)
    send(1, 0, 2, 1, 3, 4)
    for slot in range(8):
        gate_own[slot] = gate_columns(OWN, expert_at(slot))
    gate_exp[OWN] = gate_columns(OWN, expert)
    y_acc[...] = jnp.zeros_like(y_acc)
    dx_acc[...] = jnp.zeros_like(dx_acc)
    dul_acc[...] = jnp.zeros_like(dul_acc)
    ddown_acc[...] = jnp.zeros_like(ddown_acc)
    arrive_small(2)
    gate_exp[SIB] = gate_columns(SIB, expert)

    def owner(first, last):
        def body(step, carry):
            slot = first + step // 2
            rows = pl.ds(pl.multiple_of(lax.rem(step, 2) * half, half), half)
            w_ul, w_down = w_all[slot, pl.ds(0, d_model)], w_all[slot, pl.ds(d_model, ff)]
            gate = gate_own[slot, rows]
            hidden, _, d_ul = expert_math(x_all[OWN, rows], d_all[OWN, rows], gate, w_ul, w_down)
            out = nn_dot(hidden, w_down).astype(BF16).astype(F32)
            y_acc[rows] += cols(gate, d_model) * out
            dx_acc[rows] += nt_dot(d_ul, w_ul).astype(BF16).astype(F32)
            return carry

        lax.fori_loop(0, 2 * (last - first), body, 0)

    def expert_rows(slot, rows, ready=None):
        w_ul, w_down = w_all[OWN, pl.ds(0, d_model)], w_all[OWN, pl.ds(d_model, ff)]
        x_rows = x_all[slot, rows]
        hidden, u_rows, d_ul = expert_math(x_rows, d_all[slot, rows], gate_exp[slot, rows], w_ul, w_down, ready)
        dul_acc[...] += tn_dot(x_rows, d_ul)
        ddown_acc[...] += tn_dot(hidden, u_rows)

    def expert_blocks(first, stride):
        def body(step, carry):
            expert_rows(first + step * stride, pl.ds(0, tokens))
            return carry

        lax.fori_loop(0, 2, body, 0)

    arrive(0, 0, 2)
    send(0, 5, 6, 7, 8, 9, 11)
    arrive_small(0, 1)
    send_small(3, 4, 5)
    gate_exp[LEFT] = gate_columns(LEFT, expert)
    gate_exp[RIGHT] = gate_columns(RIGHT, expert)
    arrive(0, 1, 3)
    send(0, 10, 12)
    shifts[2].wait_recv()
    send(2, 4, 0, 2, 1, 3)
    arrive(0, 4)
    owner(OWN, LEFT)
    arrive(1, 0, 2)
    send(1, 5, 6, 7, 8, 9, 11)
    arrive(0, 9, 10, 11, 12)
    owner(LEFT, OPP)
    arrive(1, 1, 3)
    send(1, 10, 12)
    arrive_small(3, 4, 5)
    send_small(6)
    gate_exp[LEFT_SIB] = gate_columns(LEFT_SIB, expert)
    gate_exp[RIGHT_SIB] = gate_columns(RIGHT_SIB, expert)
    gate_exp[OPP] = gate_columns(OPP, expert)
    arrive(1, 4)
    arrive(2, 4)
    expert_blocks(OWN, 1)
    arrive(0, 5, 6, 7, 8)
    send(0, 13, 14, 15, 16)
    arrive_small(6)
    gate_exp[OPP_SIB] = gate_columns(OPP_SIB, expert)
    arrive(0, 13, 14, 15, 16)
    owner(OPP, 8)
    y_ref[...] = y_acc[...].astype(BF16)
    dx_buf[...] = dx_acc[...].astype(BF16)
    arrive(2, 0, 2)
    send(2, 5, 6, 7, 8, 9, 11)
    back = remote(dx_buf, dx_ref, shift_send.at[3], shift_recv.at[3], before)
    back.start()
    started.append(back)
    arrive(2, 1, 3)
    send(2, 10, 12)
    expert_blocks(LEFT, 2)
    arrive(1, 9, 10, 11, 12)
    arrive(2, 9, 10, 11, 12)
    expert_blocks(LEFT_SIB, 2)
    arrive(1, 5, 6, 7, 8)
    send(1, 13, 14, 15, 16)

    def prepare(slot):
        u_rows, d_hid = hidden_cotangent(d_all[slot], gate_exp[slot], w_all[OWN, pl.ds(d_model, ff)])
        u_opp[slot - OPP] = u_rows
        dh_opp[slot - OPP] = d_hid

    prepare(OPP)
    arrive(1, 13, 14, 15, 16)
    prepare(OPP_SIB)
    arrive(2, 5, 7)
    send(2, 13, 15)
    arrive(2, 6, 8)
    send(2, 14, 16)
    expert_rows(OPP, pl.ds(0, tokens), (u_opp[0], dh_opp[0]))
    arrive(2, 13, 14, 15, 16)
    expert_rows(OPP_SIB, pl.ds(0, tokens), (u_opp[1], dh_opp[1]))

    dup_ref[...] = dul_acc[:, :ff].astype(BF16)
    dlin_ref[...] = dul_acc[:, ff:].astype(BF16)
    ddown_ref[...] = ddown_acc[...].astype(BF16)
    for copy in started:
        copy.wait_send()
    back.wait_recv()


def finish_kernel(*refs):
    count = len(refs) // 2
    outs = [pltpu.make_async_copy(refs[i], refs[count + i], refs[-1].at[i]) for i in range(count)]
    for copy in outs:
        copy.start()
    for copy in outs:
        copy.wait()


def solution(mesh):
    stages = mesh.shape["stage"]
    groups = mesh.shape["expert"]
    tok_spec = P("stage", "expert", None)
    w_spec = P("stage", "expert", None, None)

    def device_step(x_act, route_idx, route_gate, w_up, w_lin, w_down, dy_out):
        _, tokens, d_model = x_act.shape
        ff = w_up.shape[-1]
        any_spec = pl.BlockSpec(memory_space=pl.ANY)
        vmem_spec = pl.BlockSpec(memory_space=pltpu.VMEM)
        dma = pltpu.SemaphoreType.DMA
        results = pl.pallas_call(
            functools.partial(moe_kernel, stages, groups),
            name="moe",
            out_shape=(
                pltpu.VMEM((tokens, d_model), BF16),
                pltpu.VMEM((tokens, d_model), BF16),
                pltpu.VMEM((d_model, ff), BF16),
                pltpu.VMEM((d_model, ff), BF16),
                pltpu.VMEM((ff, d_model), BF16),
            ),
            in_specs=[any_spec] * 7,
            out_specs=(vmem_spec,) * 5,
            scratch_shapes=[
                pltpu.VMEM((8, d_model + ff, d_model), BF16),
                pltpu.VMEM((8, tokens, d_model), BF16),
                pltpu.VMEM((8, tokens, d_model), BF16),
                pltpu.VMEM((8, 2, tokens), jnp.int32),
                pltpu.VMEM((8, 2, tokens), F32),
                pltpu.VMEM((8, tokens, 128), F32),
                pltpu.VMEM((8, tokens, 128), F32),
                pltpu.VMEM((tokens, d_model), F32),
                pltpu.VMEM((tokens, d_model), F32),
                pltpu.VMEM((tokens, d_model), BF16),
                pltpu.VMEM((d_model, 2 * ff), F32),
                pltpu.VMEM((ff, d_model), F32),
                pltpu.VMEM((2, tokens, d_model), BF16),
                pltpu.VMEM((2, tokens, ff), BF16),
                dma((4,)),
                dma((3, 17)),
                dma((3, 17)),
                dma((2, 7)),
                dma((2, 7)),
                dma((4,)),
                dma((4,)),
                pltpu.SemaphoreType.REGULAR,
                pltpu.SemaphoreType.REGULAR,
                pltpu.SemaphoreType.REGULAR,
            ],
            compiler_params=pltpu.CompilerParams(collective_id=0, has_side_effects=True, vmem_limit_bytes=60 * 1024 * 1024),
        )(x_act[0], route_idx[0].T, route_gate[0].T, w_up[0, 0], w_lin[0, 0], w_down[0, 0], dy_out[0])
        shapes = [jax.ShapeDtypeStruct(r.shape, r.dtype) for r in results]
        y_tok, dx_prev, g_up, g_lin, g_down = pl.pallas_call(
            finish_kernel,
            name="finish",
            out_shape=shapes,
            in_specs=[vmem_spec] * 5,
            out_specs=[any_spec] * 5,
            scratch_shapes=[dma((5,))],
        )(*[pltpu.with_memory_space_constraint(r, pltpu.VMEM) for r in results])
        return y_tok[None], dx_prev[None], g_up[None, None], g_lin[None, None], g_down[None, None]

    return jax.shard_map(device_step, mesh=mesh, in_specs=(tok_spec, tok_spec, tok_spec, w_spec, w_spec, w_spec, tok_spec), out_specs=(tok_spec, tok_spec, w_spec, w_spec, w_spec), check_vma=False)
```

```python
import functools

import jax
import jax.numpy as jnp
from jax import lax
from jax.experimental import pallas as pl
from jax.experimental.pallas import tpu as pltpu
from jax.sharding import PartitionSpec as P

F32 = jnp.float32
BF16 = jnp.bfloat16
MESH = pl.DeviceIdType.MESH

OWN, SIB, LEFT, LEFT_SIB, RIGHT, RIGHT_SIB, OPP, OPP_SIB = range(8)


def cols(gate, width):
    return jnp.concatenate([gate] * (width // 128), axis=1)


def nt_dot(a, b):
    return lax.dot_general(a, b, (((1,), (1,)), ((), ())), preferred_element_type=F32)


def tn_dot(a, b):
    return lax.dot_general(a, b, (((0,), (0,)), ((), ())), preferred_element_type=F32)


def nn_dot(a, b):
    return jnp.dot(a, b, preferred_element_type=F32)


def hidden_cotangent(dy_rows, gate, w_down):
    u_rows = (cols(gate, dy_rows.shape[1]) * dy_rows.astype(F32)).astype(BF16)
    return u_rows, nt_dot(u_rows, w_down).astype(BF16)


def expert_math(x_rows, dy_rows, gate, w_ul, w_down, ready=None):
    ff = w_down.shape[0]
    routed = cols(gate, ff) > 0.0
    pre = nn_dot(x_rows, w_ul)
    pre_up = jnp.where(routed, pre[:, :ff], 0.0)
    pre_lin = jnp.where(routed, pre[:, ff:], 0.0)
    sig = 1.0 / (1.0 + jnp.exp(-pre_up))
    act = pre_up * sig
    hidden = (act * pre_lin).astype(BF16)
    u_rows, d_hid = hidden_cotangent(dy_rows, gate, w_down) if ready is None else ready
    d_hid = d_hid.astype(F32)
    d_up = (d_hid * pre_lin * sig * (1.0 + pre_up * (1.0 - sig))).astype(BF16)
    d_lin = (d_hid * act).astype(BF16)
    return hidden, u_rows, jnp.concatenate([d_up, d_lin], axis=1)


def moe_kernel(
    stages, groups, x_hbm, idx_hbm, gate_hbm, up_hbm, lin_hbm, down_hbm, dy_hbm,
    y_ref, dx_ref, dup_ref, dlin_ref, ddown_ref,
    w_all, d_all, x_all, idx_all, gate_all, gate_own, gate_exp, y_acc, dx_acc, dx_buf, dul_acc, ddown_acc, u_opp, dh_opp,
    load_sem, send_sem, recv_sem, small_send, small_recv, shift_send, shift_recv, ring_ready, stage_ready, sib_ready,
):
    tokens, d_model = x_hbm.shape
    ff = down_hbm.shape[0]
    half, cut = tokens // 2, 3 * tokens // 8
    rest = half - cut
    stage, expert = lax.axis_index("stage"), lax.axis_index("expert")
    core = lax.rem(expert, 2)
    right = {"expert": lax.rem(expert + 2, groups)}
    left = {"expert": lax.rem(expert + groups - 2, groups)}
    sib = {"expert": expert + 1 - 2 * core}
    after = {"stage": lax.rem(stage + 1, stages)}
    before = {"stage": lax.rem(stage + stages - 1, stages)}

    loads = [
        pltpu.make_async_copy(up_hbm, w_all.at[OWN, pl.ds(0, d_model), pl.ds(0, ff)], load_sem.at[0]),
        pltpu.make_async_copy(lin_hbm, w_all.at[OWN, pl.ds(0, d_model), pl.ds(ff, ff)], load_sem.at[1]),
        pltpu.make_async_copy(down_hbm, w_all.at[OWN, pl.ds(d_model, ff)], load_sem.at[2]),
        pltpu.make_async_copy(dy_hbm, d_all.at[OWN], load_sem.at[3]),
    ]
    for load in loads[:3]:
        load.start()

    barrier = pltpu.get_barrier_semaphore()
    colour = lax.rem(expert // 2 + core, 2)

    def signal(sem, *peers):
        for peer in peers:
            pl.semaphore_signal(sem, inc=1, device_id=peer, device_id_type=MESH)

    @pl.when(colour == 1)
    def _():
        signal(barrier, right, left, sib, after, before)

    @pl.when(colour == 0)
    def _():
        pl.semaphore_wait(barrier, 3)
        signal(ring_ready, right, left, sib)

    @pl.when(colour == 1)
    def _():
        pl.semaphore_wait(ring_ready, 3)

    started = []

    def remote(src, dst, send, recv, peer):
        return pltpu.make_async_remote_copy(src_ref=src, dst_ref=dst, send_sem=send, recv_sem=recv, device_id=peer, device_id_type=MESH)

    arrays = (w_all, d_all, x_all)
    kinds = [
        (OWN, LEFT, 0, half, right), (OWN, LEFT, half, half, right),
        (OWN, RIGHT, half, half, left), (OWN, RIGHT, 0, half, left),
        (OWN, SIB, 0, tokens, sib),
        (LEFT, OPP, 0, cut, right), (LEFT, OPP, cut, rest, right),
        (RIGHT, OPP, tokens - cut, cut, left), (RIGHT, OPP, half, rest, left),
        (LEFT, LEFT_SIB, 0, half, sib), (LEFT, LEFT_SIB, half, half, sib),
        (RIGHT, RIGHT_SIB, half, half, sib), (RIGHT, RIGHT_SIB, 0, half, sib),
        (OPP, OPP_SIB, 0, cut, sib), (OPP, OPP_SIB, cut, rest, sib),
        (OPP, OPP_SIB, tokens - cut, cut, sib), (OPP, OPP_SIB, half, rest, sib),
    ]

    def block_copy(array, kind):
        src_slot, dst_slot, row, rows, peer = kinds[kind]
        ref = arrays[array]
        return remote(
            ref.at[src_slot, pl.ds(row, rows)], ref.at[dst_slot, pl.ds(row, rows)],
            send_sem.at[array, kind], recv_sem.at[array, kind], peer,
        )

    def send(array, *which):
        for kind in which:
            copy = block_copy(array, kind)
            copy.start()
            started.append(copy)

    def arrive(array, *which):
        for kind in which:
            block_copy(array, kind).wait_recv()

    small = [(OWN, LEFT, right), (OWN, RIGHT, left), (OWN, SIB, sib), (LEFT, OPP, right), (LEFT, LEFT_SIB, sib), (RIGHT, RIGHT_SIB, sib), (OPP, OPP_SIB, sib)]

    def small_copies(kind):
        copies = []
        for which, ref in enumerate((idx_all, gate_all)):
            src_slot, dst_slot, peer = (RIGHT, OPP, left) if (kind, which) == (3, 1) else small[kind]
            copies.append(remote(ref.at[src_slot], ref.at[dst_slot], small_send.at[which, kind], small_recv.at[which, kind], peer))
        return copies

    def send_small(*which):
        for kind in which:
            for copy in small_copies(kind):
                copy.start()
                started.append(copy)

    def arrive_small(*which):
        for kind in which:
            for copy in small_copies(kind):
                copy.wait_recv()

    for load in loads[:2]:
        load.wait()
    send(0, 0)
    loads[2].wait()
    send(0, 2, 1, 3, 4)
    loads[3].start()

    @pl.when(colour == 1)
    def _():
        pl.semaphore_wait(barrier, 2)
        signal(stage_ready, after, before)
        pl.semaphore_wait(stage_ready, 2)
        signal(sib_ready, sib)

    @pl.when(colour == 0)
    def _():
        pl.semaphore_wait(sib_ready, 1)

    shifts = [
        remote(idx_hbm, idx_all.at[OWN], shift_send.at[0], shift_recv.at[0], after),
        remote(gate_hbm, gate_all.at[OWN], shift_send.at[1], shift_recv.at[1], after),
        remote(x_hbm, x_all.at[OWN], shift_send.at[2], shift_recv.at[2], after),
    ]
    for copy in shifts:
        copy.start()
        started.append(copy)

    def gate_columns(slot, expert_id):
        ids, gates = idx_all[slot], gate_all[slot]
        row = jnp.sum(jnp.where(ids == expert_id, gates, 0.0), axis=0, keepdims=True)
        return jnp.broadcast_to(row, (128, tokens)).T

    def expert_at(slot):
        chip_step = (0, 0, groups - 2, groups - 2, 2, 2, 4, 4)[slot]
        flip = (1 - 2 * core) if slot % 2 else 0
        return lax.rem(expert + flip + chip_step, groups)

    shifts[0].wait_recv()
    shifts[1].wait_recv()
    send_small(2, 0, 1)
    loads[3].wait()
    send(1, 0, 2, 1, 3, 4)
    for slot in range(8):
        gate_own[slot] = gate_columns(OWN, expert_at(slot))
    gate_exp[OWN] = gate_columns(OWN, expert)
    y_acc[...] = jnp.zeros_like(y_acc)
    dx_acc[...] = jnp.zeros_like(dx_acc)
    dul_acc[...] = jnp.zeros_like(dul_acc)
    ddown_acc[...] = jnp.zeros_like(ddown_acc)
    arrive_small(2)
    gate_exp[SIB] = gate_columns(SIB, expert)

    def owner(first, last):
        def body(step, carry):
            slot = first + step // 2
            rows = pl.ds(pl.multiple_of(lax.rem(step, 2) * half, half), half)
            w_ul, w_down = w_all[slot, pl.ds(0, d_model)], w_all[slot, pl.ds(d_model, ff)]
            gate = gate_own[slot, rows]
            hidden, _, d_ul = expert_math(x_all[OWN, rows], d_all[OWN, rows], gate, w_ul, w_down)
            out = nn_dot(hidden, w_down).astype(BF16).astype(F32)
            y_acc[rows] += cols(gate, d_model) * out
            dx_acc[rows] += nt_dot(d_ul, w_ul).astype(BF16).astype(F32)
            return carry

        lax.fori_loop(0, 2 * (last - first), body, 0)

    def expert_rows(slot, rows, ready=None):
        w_ul, w_down = w_all[OWN, pl.ds(0, d_model)], w_all[OWN, pl.ds(d_model, ff)]
        x_rows = x_all[slot, rows]
        hidden, u_rows, d_ul = expert_math(x_rows, d_all[slot, rows], gate_exp[slot, rows], w_ul, w_down, ready)
        dul_acc[...] += tn_dot(x_rows, d_ul)
        ddown_acc[...] += tn_dot(hidden, u_rows)

    def expert_blocks(first, stride):
        def body(step, carry):
            expert_rows(first + step * stride, pl.ds(0, tokens))
            return carry

        lax.fori_loop(0, 2, body, 0)

    arrive(0, 0, 2)
    send(0, 5, 6, 7, 8, 9, 11)
    arrive_small(0, 1)
    send_small(3, 4, 5)
    gate_exp[LEFT] = gate_columns(LEFT, expert)
    gate_exp[RIGHT] = gate_columns(RIGHT, expert)
    arrive(0, 1, 3)
    send(0, 10, 12)
    shifts[2].wait_recv()
    send(2, 4, 0, 2, 1, 3)
    arrive(0, 4)
    owner(OWN, LEFT)
    arrive(1, 0, 2)
    send(1, 5, 6, 7, 8, 9, 11)
    arrive(0, 9, 10, 11, 12)
    owner(LEFT, OPP)
    arrive(1, 1, 3)
    send(1, 10, 12)
    arrive_small(3, 4, 5)
    send_small(6)
    gate_exp[LEFT_SIB] = gate_columns(LEFT_SIB, expert)
    gate_exp[RIGHT_SIB] = gate_columns(RIGHT_SIB, expert)
    gate_exp[OPP] = gate_columns(OPP, expert)
    arrive(1, 4)
    arrive(2, 4)
    expert_blocks(OWN, 1)
    arrive(0, 5, 6, 7, 8)
    send(0, 13, 14, 15, 16)
    arrive_small(6)
    gate_exp[OPP_SIB] = gate_columns(OPP_SIB, expert)
    arrive(0, 13, 14, 15, 16)
    owner(OPP, 8)
    y_ref[...] = y_acc[...].astype(BF16)
    dx_buf[...] = dx_acc[...].astype(BF16)
    arrive(2, 0, 2)
    send(2, 5, 6, 7, 8, 9, 11)
    back = remote(dx_buf, dx_ref, shift_send.at[3], shift_recv.at[3], before)
    back.start()
    started.append(back)
    arrive(2, 1, 3)
    send(2, 10, 12)
    expert_blocks(LEFT, 2)
    arrive(1, 9, 10, 11, 12)
    arrive(2, 9, 10, 11, 12)
    expert_blocks(LEFT_SIB, 2)
    arrive(1, 5, 6, 7, 8)
    send(1, 13, 14, 15, 16)

    def prepare(slot):
        u_rows, d_hid = hidden_cotangent(d_all[slot], gate_exp[slot], w_all[OWN, pl.ds(d_model, ff)])
        u_opp[slot - OPP] = u_rows
        dh_opp[slot - OPP] = d_hid

    prepare(OPP)
    arrive(1, 13, 14, 15, 16)
    prepare(OPP_SIB)
    for piece in range(4):
        arrive(2, (5, 7, 6, 8)[piece])
        send(2, (13, 15, 14, 16)[piece])
    expert_rows(OPP, pl.ds(0, tokens), (u_opp[0], dh_opp[0]))
    arrive(2, 13, 14, 15, 16)
    expert_rows(OPP_SIB, pl.ds(0, tokens), (u_opp[1], dh_opp[1]))

    dup_ref[...] = dul_acc[:, :ff].astype(BF16)
    dlin_ref[...] = dul_acc[:, ff:].astype(BF16)
    ddown_ref[...] = ddown_acc[...].astype(BF16)
    for copy in started:
        copy.wait_send()
    back.wait_recv()


def finish_kernel(*refs):
    count = len(refs) // 2
    outs = [pltpu.make_async_copy(refs[i], refs[count + i], refs[-1].at[i]) for i in range(count)]
    for copy in outs:
        copy.start()
    for copy in outs:
        copy.wait()


def solution(mesh):
    stages = mesh.shape["stage"]
    groups = mesh.shape["expert"]
    tok_spec = P("stage", "expert", None)
    w_spec = P("stage", "expert", None, None)

    def device_step(x_act, route_idx, route_gate, w_up, w_lin, w_down, dy_out):
        _, tokens, d_model = x_act.shape
        ff = w_up.shape[-1]
        any_spec = pl.BlockSpec(memory_space=pl.ANY)
        vmem_spec = pl.BlockSpec(memory_space=pltpu.VMEM)
        dma = pltpu.SemaphoreType.DMA
        results = pl.pallas_call(
            functools.partial(moe_kernel, stages, groups),
            name="moe",
            out_shape=(
                pltpu.VMEM((tokens, d_model), BF16),
                pltpu.VMEM((tokens, d_model), BF16),
                pltpu.VMEM((d_model, ff), BF16),
                pltpu.VMEM((d_model, ff), BF16),
                pltpu.VMEM((ff, d_model), BF16),
            ),
            in_specs=[any_spec] * 7,
            out_specs=(vmem_spec,) * 5,
            scratch_shapes=[
                pltpu.VMEM((8, d_model + ff, d_model), BF16),
                pltpu.VMEM((8, tokens, d_model), BF16),
                pltpu.VMEM((8, tokens, d_model), BF16),
                pltpu.VMEM((8, 2, tokens), jnp.int32),
                pltpu.VMEM((8, 2, tokens), F32),
                pltpu.VMEM((8, tokens, 128), F32),
                pltpu.VMEM((8, tokens, 128), F32),
                pltpu.VMEM((tokens, d_model), F32),
                pltpu.VMEM((tokens, d_model), F32),
                pltpu.VMEM((tokens, d_model), BF16),
                pltpu.VMEM((d_model, 2 * ff), F32),
                pltpu.VMEM((ff, d_model), F32),
                pltpu.VMEM((2, tokens, d_model), BF16),
                pltpu.VMEM((2, tokens, ff), BF16),
                dma((4,)),
                dma((3, 17)),
                dma((3, 17)),
                dma((2, 7)),
                dma((2, 7)),
                dma((4,)),
                dma((4,)),
                pltpu.SemaphoreType.REGULAR,
                pltpu.SemaphoreType.REGULAR,
                pltpu.SemaphoreType.REGULAR,
            ],
            compiler_params=pltpu.CompilerParams(collective_id=0, has_side_effects=True, vmem_limit_bytes=60 * 1024 * 1024),
        )(x_act[0], route_idx[0].T, route_gate[0].T, w_up[0, 0], w_lin[0, 0], w_down[0, 0], dy_out[0])
        shapes = [jax.ShapeDtypeStruct(r.shape, r.dtype) for r in results]
        y_tok, dx_prev, g_up, g_lin, g_down = pl.pallas_call(
            finish_kernel,
            name="finish",
            out_shape=shapes,
            in_specs=[vmem_spec] * 5,
            out_specs=[any_spec] * 5,
            scratch_shapes=[dma((5,))],
        )(*[pltpu.with_memory_space_constraint(r, pltpu.VMEM) for r in results])
        return y_tok[None], dx_prev[None], g_up[None, None], g_lin[None, None], g_down[None, None]

    return jax.shard_map(device_step, mesh=mesh, in_specs=(tok_spec, tok_spec, tok_spec, w_spec, w_spec, w_spec, tok_spec), out_specs=(tok_spec, tok_spec, w_spec, w_spec, w_spec), check_vma=False)
```

```python
import functools

import jax
import jax.numpy as jnp
from jax import lax
from jax.experimental import pallas as pl
from jax.experimental.pallas import tpu as pltpu
from jax.sharding import PartitionSpec as P

F32 = jnp.float32
BF16 = jnp.bfloat16
MESH = pl.DeviceIdType.MESH

OWN, SIB, LEFT, LEFT_SIB, RIGHT, RIGHT_SIB, OPP, OPP_SIB = range(8)


def cols(gate, width):
    return jnp.concatenate([gate] * (width // 128), axis=1)


def nt_dot(a, b):
    return lax.dot_general(a, b, (((1,), (1,)), ((), ())), preferred_element_type=F32)


def tn_dot(a, b):
    return lax.dot_general(a, b, (((0,), (0,)), ((), ())), preferred_element_type=F32)


def nn_dot(a, b):
    return jnp.dot(a, b, preferred_element_type=F32)


def hidden_cotangent(dy_rows, gate, w_down):
    u_rows = (cols(gate, dy_rows.shape[1]) * dy_rows.astype(F32)).astype(BF16)
    return u_rows, nt_dot(u_rows, w_down).astype(BF16)


def expert_math(x_rows, dy_rows, gate, w_ul, w_down, ready=None):
    ff = w_down.shape[0]
    routed = cols(gate, ff) > 0.0
    pre = nn_dot(x_rows, w_ul)
    pre_up = jnp.where(routed, pre[:, :ff], 0.0)
    pre_lin = jnp.where(routed, pre[:, ff:], 0.0)
    sig = 1.0 / (1.0 + jnp.exp(-pre_up))
    act = pre_up * sig
    hidden = (act * pre_lin).astype(BF16)
    u_rows, d_hid = hidden_cotangent(dy_rows, gate, w_down) if ready is None else ready
    d_hid = d_hid.astype(F32)
    d_up = (d_hid * pre_lin * sig * (1.0 + pre_up * (1.0 - sig))).astype(BF16)
    d_lin = (d_hid * act).astype(BF16)
    return hidden, u_rows, jnp.concatenate([d_up, d_lin], axis=1)


def moe_kernel(
    stages, groups, x_hbm, idx_hbm, gate_hbm, up_hbm, lin_hbm, down_hbm, dy_hbm,
    y_ref, dx_ref, dup_ref, dlin_ref, ddown_ref,
    w_all, d_all, x_all, idx_all, gate_all, gate_own, gate_exp, y_acc, dx_acc, dx_buf, dul_acc, ddown_acc, u_opp, dh_opp,
    load_sem, send_sem, recv_sem, small_send, small_recv, shift_send, shift_recv, ring_ready, stage_ready, sib_ready,
):
    tokens, d_model = x_hbm.shape
    ff = down_hbm.shape[0]
    half, cut = tokens // 2, 3 * tokens // 8
    rest = half - cut
    stage, expert = lax.axis_index("stage"), lax.axis_index("expert")
    core = lax.rem(expert, 2)
    right = {"expert": lax.rem(expert + 2, groups)}
    left = {"expert": lax.rem(expert + groups - 2, groups)}
    sib = {"expert": expert + 1 - 2 * core}
    after = {"stage": lax.rem(stage + 1, stages)}
    before = {"stage": lax.rem(stage + stages - 1, stages)}

    def load_rows(src, row, rows, col, sem):
        return pltpu.make_async_copy(src.at[pl.ds(row, rows)], w_all.at[OWN, pl.ds(row, rows), pl.ds(col, ff)], load_sem.at[sem])

    loads = [
        load_rows(up_hbm, 0, half, 0, 0),
        load_rows(lin_hbm, 0, half, ff, 1),
        load_rows(up_hbm, half, d_model - half, 0, 2),
        load_rows(lin_hbm, half, d_model - half, ff, 3),
        pltpu.make_async_copy(down_hbm, w_all.at[OWN, pl.ds(d_model, ff)], load_sem.at[4]),
        pltpu.make_async_copy(dy_hbm, d_all.at[OWN], load_sem.at[5]),
    ]
    for load in loads[:5]:
        load.start()

    barrier = pltpu.get_barrier_semaphore()
    colour = lax.rem(expert // 2 + core, 2)

    def signal(sem, *peers):
        for peer in peers:
            pl.semaphore_signal(sem, inc=1, device_id=peer, device_id_type=MESH)

    @pl.when(colour == 1)
    def _():
        signal(barrier, right, left, sib, after, before)

    @pl.when(colour == 0)
    def _():
        pl.semaphore_wait(barrier, 3)
        signal(ring_ready, right, left, sib)

    @pl.when(colour == 1)
    def _():
        pl.semaphore_wait(ring_ready, 3)

    started = []

    def remote(src, dst, send, recv, peer):
        return pltpu.make_async_remote_copy(src_ref=src, dst_ref=dst, send_sem=send, recv_sem=recv, device_id=peer, device_id_type=MESH)

    arrays = (w_all, d_all, x_all)
    kinds = [
        (OWN, LEFT, 0, half, right), (OWN, LEFT, half, half, right),
        (OWN, RIGHT, half, half, left), (OWN, RIGHT, 0, half, left),
        (OWN, SIB, 0, tokens, sib),
        (LEFT, OPP, 0, cut, right), (LEFT, OPP, cut, rest, right),
        (RIGHT, OPP, tokens - cut, cut, left), (RIGHT, OPP, half, rest, left),
        (LEFT, LEFT_SIB, 0, half, sib), (LEFT, LEFT_SIB, half, half, sib),
        (RIGHT, RIGHT_SIB, half, half, sib), (RIGHT, RIGHT_SIB, 0, half, sib),
        (OPP, OPP_SIB, 0, cut, sib), (OPP, OPP_SIB, cut, rest, sib),
        (OPP, OPP_SIB, tokens - cut, cut, sib), (OPP, OPP_SIB, half, rest, sib),
    ]

    def block_copy(array, kind):
        src_slot, dst_slot, row, rows, peer = kinds[kind]
        ref = arrays[array]
        return remote(
            ref.at[src_slot, pl.ds(row, rows)], ref.at[dst_slot, pl.ds(row, rows)],
            send_sem.at[array, kind], recv_sem.at[array, kind], peer,
        )

    def send(array, *which):
        for kind in which:
            copy = block_copy(array, kind)
            copy.start()
            started.append(copy)

    def arrive(array, *which):
        for kind in which:
            block_copy(array, kind).wait_recv()

    small = [(OWN, LEFT, right), (OWN, RIGHT, left), (OWN, SIB, sib), (LEFT, OPP, right), (LEFT, LEFT_SIB, sib), (RIGHT, RIGHT_SIB, sib), (OPP, OPP_SIB, sib)]

    def small_copies(kind):
        copies = []
        for which, ref in enumerate((idx_all, gate_all)):
            src_slot, dst_slot, peer = (RIGHT, OPP, left) if (kind, which) == (3, 1) else small[kind]
            copies.append(remote(ref.at[src_slot], ref.at[dst_slot], small_send.at[which, kind], small_recv.at[which, kind], peer))
        return copies

    def send_small(*which):
        for kind in which:
            for copy in small_copies(kind):
                copy.start()
                started.append(copy)

    def arrive_small(*which):
        for kind in which:
            for copy in small_copies(kind):
                copy.wait_recv()

    for load in loads[:2]:
        load.wait()
    send(0, 0)
    for load in loads[2:5]:
        load.wait()
    send(0, 2, 1, 3, 4)
    loads[5].start()

    @pl.when(colour == 1)
    def _():
        pl.semaphore_wait(barrier, 2)
        signal(stage_ready, after, before)
        pl.semaphore_wait(stage_ready, 2)
        signal(sib_ready, sib)

    @pl.when(colour == 0)
    def _():
        pl.semaphore_wait(sib_ready, 1)

    shifts = [
        remote(idx_hbm, idx_all.at[OWN], shift_send.at[0], shift_recv.at[0], after),
        remote(gate_hbm, gate_all.at[OWN], shift_send.at[1], shift_recv.at[1], after),
        remote(x_hbm, x_all.at[OWN], shift_send.at[2], shift_recv.at[2], after),
    ]
    for copy in shifts:
        copy.start()
        started.append(copy)

    def gate_columns(slot, expert_id):
        ids, gates = idx_all[slot], gate_all[slot]
        row = jnp.sum(jnp.where(ids == expert_id, gates, 0.0), axis=0, keepdims=True)
        return jnp.broadcast_to(row, (128, tokens)).T

    def expert_at(slot):
        chip_step = (0, 0, groups - 2, groups - 2, 2, 2, 4, 4)[slot]
        flip = (1 - 2 * core) if slot % 2 else 0
        return lax.rem(expert + flip + chip_step, groups)

    shifts[0].wait_recv()
    shifts[1].wait_recv()
    send_small(2, 0, 1)
    loads[5].wait()
    send(1, 0, 2, 1, 3, 4)
    for slot in range(8):
        gate_own[slot] = gate_columns(OWN, expert_at(slot))
    gate_exp[OWN] = gate_columns(OWN, expert)
    y_acc[...] = jnp.zeros_like(y_acc)
    dx_acc[...] = jnp.zeros_like(dx_acc)
    dul_acc[...] = jnp.zeros_like(dul_acc)
    ddown_acc[...] = jnp.zeros_like(ddown_acc)
    arrive_small(2)
    gate_exp[SIB] = gate_columns(SIB, expert)

    def owner(first, last):
        def body(step, carry):
            slot = first + step // 2
            rows = pl.ds(pl.multiple_of(lax.rem(step, 2) * half, half), half)
            w_ul, w_down = w_all[slot, pl.ds(0, d_model)], w_all[slot, pl.ds(d_model, ff)]
            gate = gate_own[slot, rows]
            hidden, _, d_ul = expert_math(x_all[OWN, rows], d_all[OWN, rows], gate, w_ul, w_down)
            out = nn_dot(hidden, w_down).astype(BF16).astype(F32)
            y_acc[rows] += cols(gate, d_model) * out
            dx_acc[rows] += nt_dot(d_ul, w_ul).astype(BF16).astype(F32)
            return carry

        lax.fori_loop(0, 2 * (last - first), body, 0)

    def expert_rows(slot, rows, ready=None):
        w_ul, w_down = w_all[OWN, pl.ds(0, d_model)], w_all[OWN, pl.ds(d_model, ff)]
        x_rows = x_all[slot, rows]
        hidden, u_rows, d_ul = expert_math(x_rows, d_all[slot, rows], gate_exp[slot, rows], w_ul, w_down, ready)
        dul_acc[...] += tn_dot(x_rows, d_ul)
        ddown_acc[...] += tn_dot(hidden, u_rows)

    def expert_blocks(first, stride):
        def body(step, carry):
            expert_rows(first + step * stride, pl.ds(0, tokens))
            return carry

        lax.fori_loop(0, 2, body, 0)

    arrive(0, 0, 2)
    send(0, 5, 6, 7, 8, 9, 11)
    arrive_small(0, 1)
    send_small(3, 4, 5)
    gate_exp[LEFT] = gate_columns(LEFT, expert)
    gate_exp[RIGHT] = gate_columns(RIGHT, expert)
    arrive(0, 1, 3)
    send(0, 10, 12)
    shifts[2].wait_recv()
    send(2, 4, 0, 2, 1, 3)
    arrive(0, 4)
    owner(OWN, LEFT)
    arrive(1, 0, 2)
    send(1, 5, 6, 7, 8, 9, 11)
    arrive(0, 9, 10, 11, 12)
    owner(LEFT, OPP)
    arrive(1, 1, 3)
    send(1, 10, 12)
    arrive_small(3, 4, 5)
    send_small(6)
    gate_exp[LEFT_SIB] = gate_columns(LEFT_SIB, expert)
    gate_exp[RIGHT_SIB] = gate_columns(RIGHT_SIB, expert)
    gate_exp[OPP] = gate_columns(OPP, expert)
    arrive(1, 4)
    arrive(2, 4)
    expert_blocks(OWN, 1)
    arrive(0, 5, 6, 7, 8)
    send(0, 13, 14, 15, 16)
    arrive_small(6)
    gate_exp[OPP_SIB] = gate_columns(OPP_SIB, expert)
    arrive(0, 13, 14, 15, 16)
    owner(OPP, 8)
    y_ref[...] = y_acc[...].astype(BF16)
    dx_buf[...] = dx_acc[...].astype(BF16)
    arrive(2, 0, 2)
    send(2, 5, 6, 7, 8, 9, 11)
    back = remote(dx_buf, dx_ref, shift_send.at[3], shift_recv.at[3], before)
    back.start()
    started.append(back)
    arrive(2, 1, 3)
    send(2, 10, 12)
    expert_blocks(LEFT, 2)
    arrive(1, 9, 10, 11, 12)
    arrive(2, 9, 10, 11, 12)
    expert_blocks(LEFT_SIB, 2)
    arrive(1, 5, 6, 7, 8)
    send(1, 13, 14, 15, 16)

    def prepare(slot):
        u_rows, d_hid = hidden_cotangent(d_all[slot], gate_exp[slot], w_all[OWN, pl.ds(d_model, ff)])
        u_opp[slot - OPP] = u_rows
        dh_opp[slot - OPP] = d_hid

    prepare(OPP)
    arrive(1, 13, 14, 15, 16)
    prepare(OPP_SIB)
    for piece in range(4):
        arrive(2, (5, 7, 6, 8)[piece])
        send(2, (13, 15, 14, 16)[piece])
    expert_rows(OPP, pl.ds(0, tokens), (u_opp[0], dh_opp[0]))
    arrive(2, 13, 14, 15, 16)
    expert_rows(OPP_SIB, pl.ds(0, tokens), (u_opp[1], dh_opp[1]))

    dup_ref[...] = dul_acc[:, :ff].astype(BF16)
    dlin_ref[...] = dul_acc[:, ff:].astype(BF16)
    ddown_ref[...] = ddown_acc[...].astype(BF16)
    for copy in started:
        copy.wait_send()
    back.wait_recv()


def finish_kernel(*refs):
    count = len(refs) // 2
    outs = [pltpu.make_async_copy(refs[i], refs[count + i], refs[-1].at[i]) for i in range(count)]
    for copy in outs:
        copy.start()
    for copy in outs:
        copy.wait()


def solution(mesh):
    stages = mesh.shape["stage"]
    groups = mesh.shape["expert"]
    tok_spec = P("stage", "expert", None)
    w_spec = P("stage", "expert", None, None)

    def device_step(x_act, route_idx, route_gate, w_up, w_lin, w_down, dy_out):
        _, tokens, d_model = x_act.shape
        ff = w_up.shape[-1]
        any_spec = pl.BlockSpec(memory_space=pl.ANY)
        vmem_spec = pl.BlockSpec(memory_space=pltpu.VMEM)
        dma = pltpu.SemaphoreType.DMA
        results = pl.pallas_call(
            functools.partial(moe_kernel, stages, groups),
            name="moe",
            out_shape=(
                pltpu.VMEM((tokens, d_model), BF16),
                pltpu.VMEM((tokens, d_model), BF16),
                pltpu.VMEM((d_model, ff), BF16),
                pltpu.VMEM((d_model, ff), BF16),
                pltpu.VMEM((ff, d_model), BF16),
            ),
            in_specs=[any_spec] * 7,
            out_specs=(vmem_spec,) * 5,
            scratch_shapes=[
                pltpu.VMEM((8, d_model + ff, d_model), BF16),
                pltpu.VMEM((8, tokens, d_model), BF16),
                pltpu.VMEM((8, tokens, d_model), BF16),
                pltpu.VMEM((8, 2, tokens), jnp.int32),
                pltpu.VMEM((8, 2, tokens), F32),
                pltpu.VMEM((8, tokens, 128), F32),
                pltpu.VMEM((8, tokens, 128), F32),
                pltpu.VMEM((tokens, d_model), F32),
                pltpu.VMEM((tokens, d_model), F32),
                pltpu.VMEM((tokens, d_model), BF16),
                pltpu.VMEM((d_model, 2 * ff), F32),
                pltpu.VMEM((ff, d_model), F32),
                pltpu.VMEM((2, tokens, d_model), BF16),
                pltpu.VMEM((2, tokens, ff), BF16),
                dma((6,)),
                dma((3, 17)),
                dma((3, 17)),
                dma((2, 7)),
                dma((2, 7)),
                dma((4,)),
                dma((4,)),
                pltpu.SemaphoreType.REGULAR,
                pltpu.SemaphoreType.REGULAR,
                pltpu.SemaphoreType.REGULAR,
            ],
            compiler_params=pltpu.CompilerParams(collective_id=0, has_side_effects=True, vmem_limit_bytes=60 * 1024 * 1024),
        )(x_act[0], route_idx[0].T, route_gate[0].T, w_up[0, 0], w_lin[0, 0], w_down[0, 0], dy_out[0])
        shapes = [jax.ShapeDtypeStruct(r.shape, r.dtype) for r in results]
        y_tok, dx_prev, g_up, g_lin, g_down = pl.pallas_call(
            finish_kernel,
            name="finish",
            out_shape=shapes,
            in_specs=[vmem_spec] * 5,
            out_specs=[any_spec] * 5,
            scratch_shapes=[dma((5,))],
        )(*[pltpu.with_memory_space_constraint(r, pltpu.VMEM) for r in results])
        return y_tok[None], dx_prev[None], g_up[None, None], g_lin[None, None], g_down[None, None]

    return jax.shard_map(device_step, mesh=mesh, in_specs=(tok_spec, tok_spec, tok_spec, w_spec, w_spec, w_spec, tok_spec), out_specs=(tok_spec, tok_spec, w_spec, w_spec, w_spec), check_vma=False)
```
